128 devices in a mesh: cuts: 32 (over y, z, core), rank: 4 (over x).
Axes of the slice: x: 4, y: 4, z: 4, core: 2. Of those that a mesh axis runs over, the one named last changes fastest.
Arguments:
- core_left: float32 [512, 512, 512], P('rank', 'cuts'), may hold values from -6 to 6
- core_mid: float32 [512, 512, 512], P('rank', 'cuts'), may hold values from -0.25 to 0.25
- core_right: float32 [512, 512, 512], P('rank', 'cuts'), may hold values from -6 to 6
- sketch_mid: float32 [256, 512, 256], P(None, 'cuts'), may hold values from -0.015625 to 0.015625
- sketch_right: float32 [256, 512, 256], P(None, 'cuts'), may hold values from -0.015625 to 0.015625
- tail_sketch: float32 [512, 256], replicated, may hold values from -0.25 to 0.25
- stencil: float32 [3, 512], P(None, 'cuts'), may hold values from 0.25 to 1
Outputs:
- ortho_core: float32 [512, 512, 256], P('rank', 'cuts')
- next_core: float32 [256, 512, 512], P('rank', 'cuts')
The draws below stay inside these ranges and needn't reach their ends.
All inputs are finite; a program needn't handle non-finite values.
Results may differ from the reference program's by a relative error of at most 0.00014.
Values sent between devices are 32-bit elements; how exact they have to be, the bound alone decides.
No kernel may reach another device: no remote copies, remote signals or barrier semaphores. Data moves between devices by JAX's collectives and lax.ppermute only.
A program may use at most 128 MiB of HBM per device.

```python
import math
import jax
import jax.numpy as jnp
from jax import lax

R = 512
S = 256
MODE = 512


def steps_of(rng, dims, shards, smallest, top_value):
    def one(axis_at, shards_of):
        heights = jax.random.uniform(jax.random.fold_in(jax.random.fold_in(rng, 6), axis_at), (shards_of,), jnp.float32, smallest / len(shards), top_value / len(shards))
        return jnp.repeat(jnp.exp(heights), dims[axis_at] // shards_of).reshape((-1,) + (1,) * (len(dims) - axis_at - 1))

    loudness = one(*shards[0])
    for cut in shards[1:]:
        loudness = loudness * one(*cut)
    return loudness


def noise(key, extent, spread, limit, pieces=(), dtype=jnp.bfloat16):
    factor_of = steps_of(key, extent, pieces, -0.22, 0.18) if pieces else 1.0
    array = jax.random.normal(key, extent, jnp.float32) * spread * factor_of
    return jnp.minimum(jnp.maximum(array, -limit), limit).astype(dtype)


def setup_inputs(seed: int = 0) -> dict:
    splits = jax.random.split(jax.random.key(seed), 8)
    core_left = noise(splits[0], (R, MODE, R), 1.0, 6.0, ((0, 4), (1, 32)), jnp.float32)
    core_mid = noise(splits[1], (R, MODE, R), R ** -0.5, 0.25, ((0, 4), (1, 32)), jnp.float32)
    core_right = noise(splits[2], (R, MODE, R), 1.0, 6.0, ((0, 4), (1, 32)), jnp.float32)
    sketch_mid = noise(splits[3], (S, MODE, S), (MODE * S) ** -0.5, 0.015625, ((1, 32),), jnp.float32)
    sketch_right = noise(splits[4], (S, MODE, S), (MODE * S) ** -0.5, 0.015625, ((1, 32),), jnp.float32)
    tail_sketch = noise(splits[5], (R, S), R ** -0.5, 0.25, (), jnp.float32)
    stencil = jnp.clip(0.25 + 0.75 * jax.random.uniform(splits[6], (3, MODE), jnp.float32) ** steps_of(splits[6], (3, MODE), ((1, 32),), -0.2, 0.2), 0.25, 1.0)
    return {"core_left": core_left, "core_mid": core_mid, "core_right": core_right, "sketch_mid": sketch_mid, "sketch_right": sketch_right, "tail_sketch": tail_sketch, "stencil": stencil}


HIGHEST = lax.Precision.HIGHEST

def contract_back(tt_core, right_part, sketch_core):
    left_rank, slices, right_rank = tt_core.shape
    sketch_width = sketch_core.shape[0]
    applied = jnp.dot(tt_core.reshape(left_rank * slices, right_rank).astype(jnp.float32), right_part.astype(jnp.float32), precision=HIGHEST, preferred_element_type=jnp.float32)
    applied = applied.reshape(left_rank, slices * sketch_width)
    return jnp.dot(applied.astype(jnp.float32), sketch_core.reshape(sketch_width, slices * sketch_width).T.astype(jnp.float32), precision=HIGHEST, preferred_element_type=jnp.float32)

def reference(core_left, core_mid, core_right, sketch_mid, sketch_right, tail_sketch, stencil):
    below_cells = jnp.pad(core_mid[:, :-1], ((0, 0), (1, 0), (0, 0)))
    above_cells = jnp.pad(core_mid[:, 1:], ((0, 0), (0, 1), (0, 0)))
    stepped = stencil[0][None, :, None] * below_cells + stencil[1][None, :, None] * core_mid + stencil[2][None, :, None] * above_cells
    right_sum = contract_back(core_right, tail_sketch, sketch_right)
    mid_sum = contract_back(stepped, right_sum, sketch_mid)
    flat_left = core_left.reshape(R * MODE, R)
    sketched = jnp.dot(flat_left.astype(jnp.float32), mid_sum.astype(jnp.float32), precision=HIGHEST, preferred_element_type=jnp.float32)
    gram_matrix = jnp.dot(sketched.T.astype(jnp.float32), sketched.astype(jnp.float32), precision=HIGHEST, preferred_element_type=jnp.float32)
    chol_lower = jnp.linalg.cholesky(gram_matrix)
    ortho = jax.scipy.linalg.solve_triangular(chol_lower, sketched.T, lower=True).T
    ortho_core = (ortho * math.sqrt(R * MODE)).reshape(R, MODE, S)
    project = jnp.dot(ortho.T.astype(jnp.float32), flat_left.astype(jnp.float32), precision=HIGHEST, preferred_element_type=jnp.float32)
    next_core = jnp.dot(project.astype(jnp.float32), stepped.reshape(R, MODE * R).astype(jnp.float32), precision=HIGHEST, preferred_element_type=jnp.float32)
    return (ortho_core, next_core.reshape(S, MODE, R))
```

```python
import functools
import math

import jax
import jax.numpy as jnp
from jax import lax
from jax.experimental import pallas as pl
from jax.experimental.pallas import tpu as pltpu
from jax.sharding import Mesh
from jax.sharding import PartitionSpec as P

CUTS = ("cuts_0", "cuts_1", "cuts_2")
EVERY = ("rank", "cuts_0", "cuts_1", "cuts_2")
HIGHEST = lax.Precision.HIGHEST
HIGH = lax.Precision.HIGH
F32 = jnp.float32
BF16 = jnp.bfloat16
LANES = 128
TILE = 8
BLOCK = 64

NN = (((1,), (0,)), ((), ()))
NT = (((1,), (1,)), ((), ()))
TN = (((0,), (0,)), ((), ()))


def halves(x):
    high = x.astype(BF16)
    return high, (x - high.astype(F32)).astype(BF16)


def dot3(a, b, dims):
    (ah, al), (bh, bl) = a, b
    dot = functools.partial(lax.dot_general, dimension_numbers=dims, preferred_element_type=F32)
    return dot(ah, bh) + (dot(ah, bl) + dot(al, bh))


def exact(a, b, dims):
    return lax.dot_general(a, b, dims, precision=HIGHEST, preferred_element_type=F32)


def whole_block(shape):
    return pl.BlockSpec(shape, lambda *_: (0,) * len(shape))


def contract_kernel(core_ref, part_ref, *refs):
    *sketch_refs, out_ref, applied_ref = refs
    quarters, rows, slices, width = core_ref.shape
    part = halves(part_ref[...])
    core = [core_ref[q].reshape(rows * slices, width) for q in range(quarters)]
    core = core[0] if quarters == 1 else jnp.concatenate(core, axis=1)
    applied = dot3(halves(core), part, NN)
    for h in range(len(sketch_refs)):
        applied_ref[h] = applied[:, h * LANES : (h + 1) * LANES]
    sketch_rows = sketch_refs[0].shape[0]
    sketches = [ref.reshape(sketch_rows * slices, LANES) for ref in sketch_refs]
    total = None
    for i in range(slices):
        left = [applied_ref.at[h][pl.ds(i, rows, stride=slices), :] for h in range(len(sketches))]
        right = [ref[pl.ds(i, sketch_rows, stride=slices), :] for ref in sketches]
        term = dot3(halves(jnp.concatenate(left, axis=1)), halves(jnp.concatenate(right, axis=1)), NT)
        total = term if total is None else total + term

    @pl.when(pl.program_id(0) == 0)
    def _():
        out_ref[...] = total

    @pl.when(pl.program_id(0) > 0)
    def _():
        out_ref[...] += total


def contract_back(core, part, sketch):
    quarters, rows, slices, width = core.shape
    sketch_rows, _, sketch_cols = sketch.shape
    pieces = sketch_cols // LANES
    return pl.pallas_call(
        contract_kernel,
        grid=(slices // TILE,),
        in_specs=[
            pl.BlockSpec((quarters, rows, TILE, width), lambda g: (0, 0, g, 0)),
            whole_block(part.shape),
            *[pl.BlockSpec((sketch_rows, TILE, LANES), lambda g, h=h: (0, g, h)) for h in range(pieces)],
        ],
        out_specs=whole_block((rows, sketch_rows)),
        out_shape=jax.ShapeDtypeStruct((rows, sketch_rows), F32),
        scratch_shapes=[pltpu.VMEM((pieces, rows * TILE, LANES), F32)],
        name="contract",
    )(core, part, *[sketch] * pieces)


def stencil_kernel(core_ref, below_ref, above_ref, coef_ref, out_ref):
    rows, slices, _ = core_ref.shape
    place = lax.broadcasted_iota(jnp.int32, (rows * slices, LANES), 0) % slices
    for q in range(out_ref.shape[0]):
        cols = pl.ds(q * LANES, LANES)
        core = core_ref[:, :, cols].reshape(rows * slices, LANES)
        first = jnp.broadcast_to(below_ref[:, cols][:, None, :], (rows, slices, LANES)).reshape(rows * slices, LANES)
        last = jnp.broadcast_to(above_ref[:, cols][:, None, :], (rows, slices, LANES)).reshape(rows * slices, LANES)
        below = jnp.where(place == 0, first, pltpu.roll(core, 1, 0))
        above = jnp.where(place == slices - 1, last, pltpu.roll(core, rows * slices - 1, 0))
        coef = [jnp.broadcast_to(coef_ref[k][None], (rows, slices, LANES)).reshape(rows * slices, LANES) for k in range(3)]
        stepped = coef[0] * below + coef[1] * core + coef[2] * above
        out_ref[q] = stepped.reshape(rows, slices, LANES)


def step_core(core, below, above, stencil):
    rows, slices, width = core.shape
    group = 16
    quarters = width // LANES
    coef = jnp.broadcast_to(stencil[:, :, None], (3, slices, LANES))
    return pl.pallas_call(
        stencil_kernel,
        grid=(rows // group,),
        in_specs=[
            pl.BlockSpec((group, slices, width), lambda g: (g, 0, 0)),
            pl.BlockSpec((group, width), lambda g: (g, 0)),
            pl.BlockSpec((group, width), lambda g: (g, 0)),
            whole_block(coef.shape),
        ],
        out_specs=pl.BlockSpec((quarters, group, slices, LANES), lambda g: (0, g, 0, 0)),
        out_shape=jax.ShapeDtypeStruct((quarters, rows, slices, LANES), F32),
        name="stencil",
    )(core, below, above, coef)


def invert_factor(work_ref):
    size = work_ref.shape[0]
    lane_tiles = size // LANES
    sub = lax.broadcasted_iota(jnp.int32, (TILE, LANES), 0)
    lane = lax.broadcasted_iota(jnp.int32, (TILE, LANES), 1)
    for block in range(0, size, BLOCK):
        count = BLOCK // TILE
        tiles = [
            [work_ref[pl.ds(block + t * TILE, TILE), pl.ds(h * LANES, LANES)] for h in range(lane_tiles)]
            for t in range(count)
        ]
        for p in range(count):
            k = block + p * TILE
            home, at = divmod(k, LANES)
            cols = {
                (t, j): jnp.broadcast_to(tiles[t][home][:, at + j : at + j + 1], (TILE, LANES))
                for t in range(p, count)
                for j in range(TILE)
            }
            inside = (lane >= at) & (lane < at + TILE)
            for t in range(p, count):
                fresh = jnp.where(lane - at == sub, 1.0, 0.0) if t == p else jnp.zeros((TILE, LANES), F32)
                tiles[t][home] = jnp.where(inside, fresh, tiles[t][home])
            for j in range(TILE):

                def row(x, j=j):
                    return jnp.broadcast_to(x[j : j + 1, :], (TILE, LANES))

                scale = lax.rsqrt(row(cols[p, j]))
                pivots = {jj: row(cols[p, jj]) * scale for jj in range(j + 1, TILE)}
                lines = [row(tiles[p][h]) * scale for h in range(lane_tiles)]
                for t in range(p, count):
                    m = cols[t, j] * scale
                    if t == p:
                        m = jnp.where(sub > j, m, 0.0)
                    for jj in range(j + 1, TILE):
                        cols[t, jj] = cols[t, jj] - m * pivots[jj]
                    for h in range(lane_tiles):
                        new = tiles[t][h] - m * lines[h]
                        tiles[t][h] = jnp.where(sub == j, lines[h], new) if t == p else new
        for t in range(count):
            for h in range(lane_tiles):
                work_ref[pl.ds(block + t * TILE, TILE), pl.ds(h * LANES, LANES)] = tiles[t][h]
        end = block + BLOCK
        if end < size:
            done = work_ref[pl.ds(block, BLOCK), :]
            col = lax.broadcasted_iota(jnp.int32, (size, size), 1)
            own_row = lax.broadcasted_iota(jnp.int32, (BLOCK, size), 0) + block
            own_col = lax.broadcasted_iota(jnp.int32, (BLOCK, size), 1)
            change = exact(done, jnp.where((own_col > own_row) & (own_col < end), 0.0, done), TN)
            rest = jnp.where((col >= block) & (col < end), 0.0, work_ref[...])
            rest = rest - change
            work_ref[pl.ds(end, size - end), :] = rest[end:, :]


def factor_kernel(scale, mid_ref, gram_ref, left_ref, project_ref, work_ref):
    mid = mid_ref[...]
    cross = exact(gram_ref[...], mid, NN)
    work_ref[...] = exact(mid, cross, TN)
    invert_factor(work_ref)
    row = lax.broadcasted_iota(jnp.int32, work_ref.shape, 0)
    col = lax.broadcasted_iota(jnp.int32, work_ref.shape, 1)
    inverse = jnp.where(row >= col, work_ref[...], 0.0)
    left_ref[...] = exact(mid, inverse, NT) * scale
    project_ref[...] = exact(inverse, cross, NT)


def factored(mid_sum, gram_left, scale):
    rank_width, sketch_width = mid_sum.shape
    return pl.pallas_call(
        functools.partial(factor_kernel, scale),
        out_shape=(
            jax.ShapeDtypeStruct((rank_width, sketch_width), F32),
            jax.ShapeDtypeStruct((sketch_width, rank_width), F32),
        ),
        scratch_shapes=[pltpu.VMEM((sketch_width, sketch_width), F32)],
        name="factor",
    )(mid_sum, gram_left)


def apply_kernel(rows_ref, right_ref, out_ref):
    out_ref[...] = dot3(halves(rows_ref[...]), halves(right_ref[...]), NN)


def apply_right(rows, right):
    count, depth = rows.shape
    width = right.shape[1]
    group = 512
    return pl.pallas_call(
        apply_kernel,
        grid=(count // group,),
        in_specs=[pl.BlockSpec((group, depth), lambda g: (g, 0)), whole_block(right.shape)],
        out_specs=pl.BlockSpec((group, width), lambda g: (g, 0)),
        out_shape=jax.ShapeDtypeStruct((count, width), F32),
        name="ortho",
    )(rows, right)


def project_kernel(project_ref, stepped_ref, out_ref):
    depth, slices, _ = stepped_ref.shape
    rows = project_ref.shape[0]
    project = halves(project_ref[...])
    stepped = stepped_ref.reshape(depth * slices, LANES)
    out = out_ref.reshape(rows * slices, LANES)
    for i in range(0, slices, 2):
        pair = jnp.concatenate([stepped[pl.ds(i + d, depth, stride=slices), :] for d in range(2)], axis=1)
        product = dot3(project, halves(pair), NN)
        for d in range(2):
            out[pl.ds(i + d, rows, stride=slices), :] = product[:, d * LANES : (d + 1) * LANES]


def projected(project, stepped):
    depth, slices, _ = stepped.shape
    rows = project.shape[0]
    return pl.pallas_call(
        project_kernel,
        grid=(slices // TILE,),
        in_specs=[whole_block(project.shape), pl.BlockSpec((depth, TILE, LANES), lambda g: (0, g, 0))],
        out_specs=pl.BlockSpec((rows, TILE, LANES), lambda g: (0, g, 0)),
        out_shape=jax.ShapeDtypeStruct((rows, slices, LANES), F32),
        name="project",
    )(project, stepped)


def summed_lines(partial, axes):
    peers = lax.axis_size(axes)
    blocks = partial.reshape(peers, -1, partial.shape[-1])
    return jnp.sum(lax.all_to_all(blocks, axes, 0, 0, tiled=True), axis=0)


def whole_of(lines):
    copies = jnp.broadcast_to(lines, (lax.axis_size(EVERY), *lines.shape))
    return lax.all_to_all(copies, EVERY, 0, 0, tiled=True).reshape(-1, lines.shape[-1])


def neighbours(core):
    count = lax.axis_size(CUTS)
    head, tail = core[:, 0, :], core[:, -1, :]
    below = lax.ppermute(tail, CUTS, [(i, i + 1) for i in range(count - 1)])
    above = lax.ppermute(head, CUTS, [(i + 1, i) for i in range(count - 1)])
    return below, above


def shards(core_left, core_mid, core_right, sketch_mid, sketch_right, tail_sketch, stencil):
    row_count, slices, rank_width = core_left.shape
    sketch_width = tail_sketch.shape[1]
    quarters = rank_width // LANES
    ranks = lax.axis_size("rank")

    below, above = neighbours(core_mid)
    right_part = contract_back(core_right[None], tail_sketch, sketch_right)
    stepped = step_core(core_mid, below, above, stencil)
    right_sum = whole_of(summed_lines(right_part, CUTS))

    own_cols = lax.all_to_all(stepped, "rank", 0, 0, tiled=True)

    flat_left = core_left.reshape(row_count * slices, rank_width)
    local_gram = lax.dot_general(flat_left, flat_left, TN, precision=HIGH, preferred_element_type=F32)
    gram_left = whole_of(summed_lines(local_gram, EVERY))

    mid_sum = whole_of(summed_lines(contract_back(stepped, right_sum, sketch_mid), CUTS))

    scale = math.sqrt(rank_width * slices * lax.axis_size(CUTS))
    left, project = factored(mid_sum, gram_left, scale)

    product = projected(project, own_cols.reshape(rank_width, slices, LANES))
    blocks = product.reshape(ranks, sketch_width // ranks, slices, LANES)
    arrived = lax.all_to_all(blocks, "rank", 0, 0, tiled=True)
    next_core = jnp.moveaxis(arrived, 0, 2).reshape(sketch_width // ranks, slices, quarters * LANES)

    ortho_core = apply_right(flat_left, left).reshape(row_count, slices, sketch_width)
    return ortho_core, next_core


def solution(mesh):
    split = Mesh(
        mesh.devices.reshape(4, 4, 2, mesh.shape["rank"]), ("cuts_0", "cuts_1", "cuts_2", "rank")
    )
    in_specs = (
        P("rank", CUTS, None),
        P("rank", CUTS, None),
        P("rank", CUTS, None),
        P(None, CUTS, None),
        P(None, CUTS, None),
        P(),
        P(None, CUTS),
    )
    out_specs = (P("rank", CUTS, None), P("rank", CUTS, None))
    return jax.shard_map(
        shards, mesh=split, in_specs=in_specs, out_specs=out_specs, check_vma=False
    )
```

```python
import functools
import math

import jax
import jax.numpy as jnp
from jax import lax
from jax.experimental import pallas as pl
from jax.experimental.pallas import tpu as pltpu
from jax.sharding import Mesh
from jax.sharding import PartitionSpec as P

CUTS = ("cuts_0", "cuts_1", "cuts_2")
EVERY = ("rank", "cuts_0", "cuts_1", "cuts_2")
HIGHEST = lax.Precision.HIGHEST
F32 = jnp.float32
BF16 = jnp.bfloat16
LANES = 128
TILE = 8
BLOCK = 64
PIECES = (1, 1, 2, 1)

NN = (((1,), (0,)), ((), ()))
NT = (((1,), (1,)), ((), ()))
TN = (((0,), (0,)), ((), ()))


def halves(x):
    high = x.astype(BF16)
    return high, (x - high.astype(F32)).astype(BF16)


def dot3(a, b, dims):
    (ah, al), (bh, bl) = a, b
    dot = functools.partial(lax.dot_general, dimension_numbers=dims, preferred_element_type=F32)
    return dot(ah, bh) + (dot(ah, bl) + dot(al, bh))


def exact(a, b, dims):
    return lax.dot_general(a, b, dims, precision=HIGHEST, preferred_element_type=F32)


def whole_block(shape):
    return pl.BlockSpec(shape, lambda *_: (0,) * len(shape))


def own_block(rank_ref, distance, ranks):
    return pl.multiple_of(lax.rem(rank_ref[0] + distance, ranks) * LANES, LANES)


def contract_kernel(core_parts, rank_ref, part_ref, *refs):
    count = sum(core_parts) if core_parts else 1
    core_refs, (*sketch_refs, out_ref, applied_ref) = list(refs[:count]), refs[count:]
    slices = core_refs[0].shape[1]
    if not core_parts:
        core = core_refs[0][...].reshape(-1, core_refs[0].shape[2])
        part = part_ref[...]
    else:
        blocks, lines = [], []
        for distance, pieces in enumerate(core_parts):
            taken = [core_refs.pop(0)[...].reshape(-1, LANES) for _ in range(pieces)]
            blocks.append(taken[0] if pieces == 1 else jnp.concatenate(taken, axis=0))
            lines.append(part_ref[pl.ds(own_block(rank_ref, distance, len(core_parts)), LANES), :])
        core, part = jnp.concatenate(blocks, axis=1), jnp.concatenate(lines, axis=0)
    rows = core.shape[0] // slices
    applied = dot3(halves(core), halves(part), NN)
    for h in range(len(sketch_refs)):
        applied_ref[h] = applied[:, h * LANES : (h + 1) * LANES]
    sketch_rows = sketch_refs[0].shape[0]
    sketches = [ref.reshape(sketch_rows * slices, LANES) for ref in sketch_refs]
    total = None
    for i in range(slices):
        left = [applied_ref.at[h][pl.ds(i, rows, stride=slices), :] for h in range(len(sketches))]
        right = [ref[pl.ds(i, sketch_rows, stride=slices), :] for ref in sketches]
        term = dot3(halves(jnp.concatenate(left, axis=1)), halves(jnp.concatenate(right, axis=1)), NT)
        total = term if total is None else total + term

    @pl.when(pl.program_id(0) == 0)
    def _():
        out_ref[...] = total

    @pl.when(pl.program_id(0) > 0)
    def _():
        out_ref[...] += total


SCALAR = pl.BlockSpec(memory_space=pltpu.SMEM)


def contract_back(rank, cores, core_parts, part, sketch):
    slices = cores[0].shape[1]
    sketch_rows, _, sketch_cols = sketch.shape
    rows = sum(core.shape[0] for core in cores[: core_parts[0] if core_parts else 1])
    pieces = sketch_cols // LANES
    return pl.pallas_call(
        functools.partial(contract_kernel, core_parts),
        grid=(slices // TILE,),
        in_specs=[
            SCALAR,
            whole_block(part.shape),
            *[pl.BlockSpec((core.shape[0], TILE, core.shape[2]), lambda g: (0, g, 0)) for core in cores],
            *[pl.BlockSpec((sketch_rows, TILE, LANES), lambda g, h=h: (0, g, h)) for h in range(pieces)],
        ],
        out_specs=whole_block((rows, sketch_rows)),
        out_shape=jax.ShapeDtypeStruct((rows, sketch_rows), F32),
        scratch_shapes=[pltpu.VMEM((pieces, rows * TILE, LANES), F32)],
        name="contract",
    )(rank, part, *cores, *[sketch] * pieces)


def stencil_kernel(pieces, rank_ref, core_ref, below_ref, above_ref, coef_ref, *out_refs):
    rows, slices, _ = core_ref.shape
    out_refs = list(out_refs)
    place = lax.broadcasted_iota(jnp.int32, (rows * slices, LANES), 0) % slices
    coef = [jnp.broadcast_to(coef_ref[k][None], (rows, slices, LANES)).reshape(rows * slices, LANES) for k in range(3)]
    for distance, count in enumerate(pieces):
        cols = pl.ds(own_block(rank_ref, distance, len(pieces)), LANES)
        core = core_ref[:, :, cols].reshape(rows * slices, LANES)
        first = jnp.broadcast_to(below_ref[:, cols][:, None, :], (rows, slices, LANES)).reshape(rows * slices, LANES)
        last = jnp.broadcast_to(above_ref[:, cols][:, None, :], (rows, slices, LANES)).reshape(rows * slices, LANES)
        below = jnp.where(place == 0, first, pltpu.roll(core, 1, 0))
        above = jnp.where(place == slices - 1, last, pltpu.roll(core, rows * slices - 1, 0))
        stepped = (coef[0] * below + coef[1] * core + coef[2] * above).reshape(rows, slices, LANES)
        each = pl.num_programs(0) // count
        for n in range(count):
            out_ref = out_refs.pop(0)
            if count == 1:
                out_ref[...] = stepped
                continue

            @pl.when(pl.program_id(0) // each == n)
            def _(out_ref=out_ref, stepped=stepped):
                out_ref[...] = stepped


def step_core(rank, core, below, above, stencil, pieces):
    rows, slices, width = core.shape
    group = 16
    coef = jnp.broadcast_to(stencil[:, :, None], (3, slices, LANES))
    out_specs, out_shape = [], []
    for count in pieces:
        each = rows // group // count
        for n in range(count):
            out_specs.append(
                pl.BlockSpec(
                    (group, slices, LANES), lambda g, n=n, each=each: (jnp.clip(g - n * each, 0, each - 1), 0, 0)
                )
            )
            out_shape.append(jax.ShapeDtypeStruct((rows // count, slices, LANES), F32))
    return pl.pallas_call(
        functools.partial(stencil_kernel, pieces),
        grid=(rows // group,),
        in_specs=[
            SCALAR,
            pl.BlockSpec((group, slices, width), lambda g: (g, 0, 0)),
            pl.BlockSpec((group, width), lambda g: (g, 0)),
            pl.BlockSpec((group, width), lambda g: (g, 0)),
            whole_block(coef.shape),
        ],
        out_specs=out_specs,
        out_shape=out_shape,
        name="stencil",
    )(rank, core, below, above, coef)


def invert_factor(work_ref):
    size = work_ref.shape[0]
    lane_tiles = size // LANES
    sub = lax.broadcasted_iota(jnp.int32, (TILE, LANES), 0)
    lane = lax.broadcasted_iota(jnp.int32, (TILE, LANES), 1)
    for block in range(0, size, BLOCK):
        count = BLOCK // TILE
        tiles = [
            [work_ref[pl.ds(block + t * TILE, TILE), pl.ds(h * LANES, LANES)] for h in range(lane_tiles)]
            for t in range(count)
        ]
        for p in range(count):
            k = block + p * TILE
            home, at = divmod(k, LANES)
            cols = {
                (t, j): jnp.broadcast_to(tiles[t][home][:, at + j : at + j + 1], (TILE, LANES))
                for t in range(p, count)
                for j in range(TILE)
            }
            inside = (lane >= at) & (lane < at + TILE)
            for t in range(p, count):
                fresh = jnp.where(lane - at == sub, 1.0, 0.0) if t == p else jnp.zeros((TILE, LANES), F32)
                tiles[t][home] = jnp.where(inside, fresh, tiles[t][home])
            for j in range(TILE):

                def row(x, j=j):
                    return jnp.broadcast_to(x[j : j + 1, :], (TILE, LANES))

                scale = lax.rsqrt(row(cols[p, j]))
                pivots = {jj: row(cols[p, jj]) * scale for jj in range(j + 1, TILE)}
                lines = [row(tiles[p][h]) * scale for h in range(lane_tiles)]
                for t in range(p, count):
                    m = cols[t, j] * scale
                    if t == p:
                        m = jnp.where(sub > j, m, 0.0)
                    for jj in range(j + 1, TILE):
                        cols[t, jj] = cols[t, jj] - m * pivots[jj]
                    for h in range(lane_tiles):
                        new = tiles[t][h] - m * lines[h]
                        tiles[t][h] = jnp.where(sub == j, lines[h], new) if t == p else new
        for t in range(count):
            for h in range(lane_tiles):
                work_ref[pl.ds(block + t * TILE, TILE), pl.ds(h * LANES, LANES)] = tiles[t][h]
        end = block + BLOCK
        if end < size:
            done = work_ref[pl.ds(block, BLOCK), :]
            col = lax.broadcasted_iota(jnp.int32, (size, size), 1)
            own_row = lax.broadcasted_iota(jnp.int32, (BLOCK, size), 0) + block
            own_col = lax.broadcasted_iota(jnp.int32, (BLOCK, size), 1)
            change = exact(done, jnp.where((own_col > own_row) & (own_col < end), 0.0, done), TN)
            rest = jnp.where((col >= block) & (col < end), 0.0, work_ref[...])
            rest = rest - change
            work_ref[pl.ds(end, size - end), :] = rest[end:, :]


def factor_kernel(scale, mid_ref, gram_ref, left_ref, project_ref, work_ref):
    mid = mid_ref[...]
    half = mid.shape[0] // 2
    upper, lower = mid[:half], mid[half:]
    side = gram_ref[:half, half:]
    corner = jnp.concatenate([gram_ref[half:, :half], gram_ref[half:, half:]], axis=0)
    cross = jnp.concatenate(
        [
            exact(gram_ref[:half, :half], upper, NN) + exact(side, lower, NN),
            exact(side, upper, TN) + exact(corner, lower, NN),
        ],
        axis=0,
    )
    work_ref[...] = exact(mid, cross, TN)
    invert_factor(work_ref)
    row = lax.broadcasted_iota(jnp.int32, work_ref.shape, 0)
    col = lax.broadcasted_iota(jnp.int32, work_ref.shape, 1)
    inverse = jnp.where(row >= col, work_ref[...], 0.0)
    left_ref[...] = exact(mid, inverse, NT) * scale
    project_ref[...] = exact(inverse, cross, NT)


def factored(mid_sum, gram_left, scale):
    rank_width, sketch_width = mid_sum.shape
    return pl.pallas_call(
        functools.partial(factor_kernel, scale),
        out_shape=(
            jax.ShapeDtypeStruct((rank_width, sketch_width), F32),
            jax.ShapeDtypeStruct((sketch_width, rank_width), F32),
        ),
        scratch_shapes=[pltpu.VMEM((sketch_width, sketch_width), F32)],
        name="factor",
    )(mid_sum, gram_left)


def gram_kernel(rows_ref, out_ref):
    half = rows_ref.shape[1] // 2
    high, low = halves(rows_ref[...])
    first = (high[:, :half], low[:, :half])
    second = (high[:, half:], low[:, half:])
    top = dot3(first, (high, low), TN)
    corner = dot3(second, second, TN)
    corner = jnp.concatenate([corner[: half // 2], corner[half // 2 :]], axis=1)
    total = jnp.concatenate([top, corner], axis=0)

    @pl.when(pl.program_id(0) == 0)
    def _():
        out_ref[...] = total

    @pl.when(pl.program_id(0) > 0)
    def _():
        out_ref[...] += total


def packed_gram(rows):
    count, depth = rows.shape
    group = 512
    shape = (depth // 2 + depth // 4, depth)
    return pl.pallas_call(
        gram_kernel,
        grid=(count // group,),
        in_specs=[pl.BlockSpec((group, depth), lambda g: (g, 0))],
        out_specs=whole_block(shape),
        out_shape=jax.ShapeDtypeStruct(shape, F32),
        name="gram",
    )(rows)


def apply_kernel(rows_ref, right_ref, out_ref):
    out_ref[...] = dot3(halves(rows_ref[...]), halves(right_ref[...]), NN)


def apply_right(rows, right):
    count, depth = rows.shape
    width = right.shape[1]
    group = 512
    return pl.pallas_call(
        apply_kernel,
        grid=(count // group,),
        in_specs=[pl.BlockSpec((group, depth), lambda g: (g, 0)), whole_block(right.shape)],
        out_specs=pl.BlockSpec((group, width), lambda g: (g, 0)),
        out_shape=jax.ShapeDtypeStruct((count, width), F32),
        name="ortho",
    )(rows, right)


def project_kernel(pieces, rank_ref, project_ref, *refs):
    *stepped_refs, out_ref = refs
    slices = stepped_refs[0].shape[1]
    rows = project_ref.shape[0]
    ranks = len(pieces)
    project = halves(
        jnp.concatenate(
            [project_ref[:, pl.ds(own_block(rank_ref, ranks - distance, ranks), LANES)] for distance in range(ranks)],
            axis=1,
        )
    )
    stepped = [(ref.reshape(-1, LANES), ref.shape[0]) for ref in stepped_refs]
    out = out_ref.reshape(rows * slices, LANES)

    def slab(i):
        return jnp.concatenate([ref[pl.ds(i, count, stride=slices), :] for ref, count in stepped], axis=0)

    for i in range(0, slices, 2):
        product = dot3(project, halves(jnp.concatenate([slab(i), slab(i + 1)], axis=1)), NN)
        for d in range(2):
            out[pl.ds(i + d, rows, stride=slices), :] = product[:, d * LANES : (d + 1) * LANES]


def projected(rank, project, stepped, pieces):
    slices = stepped[0].shape[1]
    rows = project.shape[0]
    return pl.pallas_call(
        functools.partial(project_kernel, pieces),
        grid=(slices // TILE,),
        in_specs=[
            SCALAR,
            whole_block(project.shape),
            *[pl.BlockSpec((block.shape[0], TILE, LANES), lambda g: (0, g, 0)) for block in stepped],
        ],
        out_specs=pl.BlockSpec((rows, TILE, LANES), lambda g: (0, g, 0)),
        out_shape=jax.ShapeDtypeStruct((rows, slices, LANES), F32),
        name="project",
    )(rank, project, *stepped)


def summed_lines(partial, axes):
    peers = lax.axis_size(axes)
    blocks = partial.reshape(peers, -1, partial.shape[-1])
    return jnp.sum(lax.all_to_all(blocks, axes, 0, 0, tiled=True), axis=0)


def copies_of(lines, axes):
    copies = jnp.broadcast_to(lines, (lax.axis_size(axes), *lines.shape))
    return lax.all_to_all(copies, axes, 0, 0, tiled=True)


def whole_of(lines, axes):
    return copies_of(lines, axes).reshape(-1, lines.shape[-1])


def shifted(array, distance):
    count = lax.axis_size("rank")
    return lax.ppermute(array, "rank", [(i, (i + distance) % count) for i in range(count)])


def neighbours(core):
    count = lax.axis_size(CUTS)
    head, tail = core[:, 0, :], core[:, -1, :]
    below = lax.ppermute(tail, CUTS, [(i, i + 1) for i in range(count - 1)])
    above = lax.ppermute(head, CUTS, [(i + 1, i) for i in range(count - 1)])
    return below, above


def step(core_left, core_mid, core_right, sketch_mid, sketch_right, tail_sketch, stencil):
    row_count, slices, rank_width = core_left.shape
    sketch_width = tail_sketch.shape[1]
    quarters = rank_width // LANES
    ranks = lax.axis_size("rank")
    flat_left = core_left.reshape(row_count * slices, rank_width)

    rank = lax.axis_index("rank").astype(jnp.int32).reshape(1)

    below, above = neighbours(core_mid)
    stepped = step_core(rank, core_mid, below, above, stencil, PIECES)
    own, up, far_up, far_down, down = stepped
    up = shifted(up, 1)
    down = shifted(down, -1)
    far_up = shifted(far_up, 1)
    far_down = shifted(far_down, -1)
    far_up = shifted(far_up, 1)
    far_down = shifted(far_down, -1)

    gram_left = packed_gram(flat_left)
    gram_left = summed_lines(gram_left, CUTS)
    gram_left = sum([shifted(gram_left, d) for d in range(1, ranks)], gram_left)
    gram_left = whole_of(gram_left, CUTS)

    right_part = contract_back(rank, [core_right], (), tail_sketch, sketch_right)
    right_sum = summed_lines(right_part, CUTS)
    right_sum = whole_of(right_sum, EVERY)

    mid_part = contract_back(rank, stepped, PIECES, right_sum, sketch_mid)
    mid_sum = summed_lines(mid_part, CUTS)
    mid_sum = whole_of(mid_sum, EVERY)

    scale = math.sqrt(rank_width * slices * lax.axis_size(CUTS))
    left, project = factored(mid_sum, gram_left, scale)
    product = projected(rank, project, [own, up, far_up, far_down, down], PIECES)
    blocks = product.reshape(ranks, sketch_width // ranks, slices, LANES)
    arrived = lax.all_to_all(blocks, "rank", 0, 0, tiled=True)
    next_core = jnp.moveaxis(arrived, 0, 2).reshape(sketch_width // ranks, slices, quarters * LANES)
    ortho_core = apply_right(flat_left, left).reshape(row_count, slices, sketch_width)
    return ortho_core, next_core


def solution(mesh):
    split = Mesh(
        mesh.devices.reshape(4, 4, 2, mesh.shape["rank"]), ("cuts_0", "cuts_1", "cuts_2", "rank")
    )
    in_specs = (
        P("rank", CUTS, None),
        P("rank", CUTS, None),
        P("rank", CUTS, None),
        P(None, CUTS, None),
        P(None, CUTS, None),
        P(),
        P(None, CUTS),
    )
    out_specs = (P("rank", CUTS, None), P("rank", CUTS, None))
    return jax.shard_map(step, mesh=split, in_specs=in_specs, out_specs=out_specs, check_vma=False)
```

```python
import functools
import math

import jax
import jax.numpy as jnp
from jax import lax
from jax.experimental import pallas as pl
from jax.experimental.pallas import tpu as pltpu
from jax.sharding import Mesh
from jax.sharding import PartitionSpec as P

CUTS = ("cuts_0", "cuts_1", "cuts_2")
EVERY = ("rank", "cuts_0", "cuts_1", "cuts_2")
HIGHEST = lax.Precision.HIGHEST
F32 = jnp.float32
BF16 = jnp.bfloat16
LANES = 128
TILE = 8
BLOCK = 64
PIECES = (1, 1, 2, 1)

NN = (((1,), (0,)), ((), ()))
NT = (((1,), (1,)), ((), ()))
TN = (((0,), (0,)), ((), ()))


def halves(x):
    high = x.astype(BF16)
    return high, (x - high.astype(F32)).astype(BF16)


def dot3(a, b, dims):
    (ah, al), (bh, bl) = a, b
    dot = functools.partial(lax.dot_general, dimension_numbers=dims, preferred_element_type=F32)
    return dot(ah, bh) + (dot(ah, bl) + dot(al, bh))


def exact(a, b, dims):
    return lax.dot_general(a, b, dims, precision=HIGHEST, preferred_element_type=F32)


def whole_block(shape):
    return pl.BlockSpec(shape, lambda *_: (0,) * len(shape))


def own_block(rank_ref, distance, ranks):
    return pl.multiple_of(lax.rem(rank_ref[0] + distance, ranks) * LANES, LANES)


def spread(out_ref, total):
    peers, height, _ = out_ref.shape
    out = out_ref.reshape(peers * height, LANES)
    lines = total.shape[0] // peers
    for h in range(total.shape[1] // LANES):
        for j in range(lines):
            block = total[j * peers : (j + 1) * peers, h * LANES : (h + 1) * LANES]
            out[pl.ds(h * lines + j, peers, stride=height), :] = block


def gathered(ref, peers, lines, first=0):
    count, height, _ = ref.shape
    flat = ref.reshape(count * height, LANES)
    return jnp.concatenate(
        [
            jnp.concatenate(
                [flat[pl.ds(first * height + h * lines + j, peers, stride=height), :] for h in range(height // lines)],
                axis=1,
            )
            for j in range(lines)
        ],
        axis=0,
    )


def contract_kernel(core_parts, rank_ref, part_ref, *refs):
    count = sum(core_parts) if core_parts else 1
    core_refs, (*sketch_refs, out_ref, applied_ref, sum_ref) = list(refs[:count]), refs[count:]
    peers = out_ref.shape[0]
    slices = core_refs[0].shape[1]
    if not core_parts:
        core = core_refs[0][...].reshape(-1, core_refs[0].shape[2])
        part = part_ref[...]
    else:
        blocks, lines = [], []
        for distance, pieces in enumerate(core_parts):
            taken = [core_refs.pop(0)[...].reshape(-1, LANES) for _ in range(pieces)]
            blocks.append(taken[0] if pieces == 1 else jnp.concatenate(taken, axis=0))
            block = lax.rem(rank_ref[0] + distance, len(core_parts))
            lines.append(gathered(part_ref, peers, LANES // peers, block * peers))
        core, part = jnp.concatenate(blocks, axis=1), jnp.concatenate(lines, axis=0)
    rows = core.shape[0] // slices
    applied = dot3(halves(core), halves(part), NN)
    for h in range(len(sketch_refs)):
        applied_ref[h] = applied[:, h * LANES : (h + 1) * LANES]
    sketch_rows = sketch_refs[0].shape[0]
    sketches = [ref.reshape(sketch_rows * slices, LANES) for ref in sketch_refs]
    total = None
    for i in range(slices):
        left = [applied_ref.at[h][pl.ds(i, rows, stride=slices), :] for h in range(len(sketches))]
        right = [ref[pl.ds(i, sketch_rows, stride=slices), :] for ref in sketches]
        term = dot3(halves(jnp.concatenate(left, axis=1)), halves(jnp.concatenate(right, axis=1)), NT)
        total = term if total is None else total + term

    last = pl.num_programs(0) - 1

    @pl.when(pl.program_id(0) == 0)
    def _():
        sum_ref[...] = total

    @pl.when((pl.program_id(0) > 0) & (pl.program_id(0) < last))
    def _():
        sum_ref[...] += total

    @pl.when(pl.program_id(0) == last)
    def _():
        spread(out_ref, sum_ref[...] + total)


SCALAR = pl.BlockSpec(memory_space=pltpu.SMEM)


def contract_back(rank, cores, core_parts, part, sketch):
    slices = cores[0].shape[1]
    sketch_rows, _, sketch_cols = sketch.shape
    rows = sum(core.shape[0] for core in cores[: core_parts[0] if core_parts else 1])
    pieces = sketch_cols // LANES
    peers = lax.axis_size(CUTS)
    shape = (peers, rows * sketch_rows // LANES // peers, LANES)
    return pl.pallas_call(
        functools.partial(contract_kernel, core_parts),
        grid=(slices // TILE,),
        in_specs=[
            SCALAR,
            whole_block(part.shape),
            *[pl.BlockSpec((core.shape[0], TILE, core.shape[2]), lambda g: (0, g, 0)) for core in cores],
            *[pl.BlockSpec((sketch_rows, TILE, LANES), lambda g, h=h: (0, g, h)) for h in range(pieces)],
        ],
        out_specs=whole_block(shape),
        out_shape=jax.ShapeDtypeStruct(shape, F32),
        scratch_shapes=[pltpu.VMEM((pieces, rows * TILE, LANES), F32), pltpu.VMEM((rows, sketch_rows), F32)],
        name="contract",
    )(rank, part, *cores, *[sketch] * pieces)


def stencil_kernel(pieces, rank_ref, core_ref, below_ref, above_ref, coef_ref, *out_refs):
    rows, slices, _ = core_ref.shape
    out_refs = list(out_refs)
    place = lax.broadcasted_iota(jnp.int32, (rows * slices, LANES), 0) % slices
    coef = [jnp.broadcast_to(coef_ref[k][None], (rows, slices, LANES)).reshape(rows * slices, LANES) for k in range(3)]
    for distance, count in enumerate(pieces):
        cols = pl.ds(own_block(rank_ref, distance, len(pieces)), LANES)
        core = core_ref[:, :, cols].reshape(rows * slices, LANES)
        first = jnp.broadcast_to(below_ref[:, cols][:, None, :], (rows, slices, LANES)).reshape(rows * slices, LANES)
        last = jnp.broadcast_to(above_ref[:, cols][:, None, :], (rows, slices, LANES)).reshape(rows * slices, LANES)
        below = jnp.where(place == 0, first, pltpu.roll(core, 1, 0))
        above = jnp.where(place == slices - 1, last, pltpu.roll(core, rows * slices - 1, 0))
        stepped = (coef[0] * below + coef[1] * core + coef[2] * above).reshape(rows, slices, LANES)
        each = pl.num_programs(0) // count
        for n in range(count):
            out_ref = out_refs.pop(0)
            if count == 1:
                out_ref[...] = stepped
                continue

            @pl.when(pl.program_id(0) // each == n)
            def _(out_ref=out_ref, stepped=stepped):
                out_ref[...] = stepped


def step_core(rank, core, below, above, stencil, pieces):
    rows, slices, width = core.shape
    group = 16
    coef = jnp.broadcast_to(stencil[:, :, None], (3, slices, LANES))
    out_specs, out_shape = [], []
    for count in pieces:
        each = rows // group // count
        for n in range(count):
            out_specs.append(
                pl.BlockSpec(
                    (group, slices, LANES), lambda g, n=n, each=each: (jnp.clip(g - n * each, 0, each - 1), 0, 0)
                )
            )
            out_shape.append(jax.ShapeDtypeStruct((rows // count, slices, LANES), F32))
    return pl.pallas_call(
        functools.partial(stencil_kernel, pieces),
        grid=(rows // group,),
        in_specs=[
            SCALAR,
            pl.BlockSpec((group, slices, width), lambda g: (g, 0, 0)),
            pl.BlockSpec((group, width), lambda g: (g, 0)),
            pl.BlockSpec((group, width), lambda g: (g, 0)),
            whole_block(coef.shape),
        ],
        out_specs=out_specs,
        out_shape=out_shape,
        name="stencil",
    )(rank, core, below, above, coef)


def invert_factor(work_ref):
    size = work_ref.shape[0]
    lane_tiles = size // LANES
    sub = lax.broadcasted_iota(jnp.int32, (TILE, LANES), 0)
    lane = lax.broadcasted_iota(jnp.int32, (TILE, LANES), 1)
    for block in range(0, size, BLOCK):
        count = BLOCK // TILE
        tiles = [
            [work_ref[pl.ds(block + t * TILE, TILE), pl.ds(h * LANES, LANES)] for h in range(lane_tiles)]
            for t in range(count)
        ]
        for p in range(count):
            k = block + p * TILE
            home, at = divmod(k, LANES)
            cols = {
                (t, j): jnp.broadcast_to(tiles[t][home][:, at + j : at + j + 1], (TILE, LANES))
                for t in range(p, count)
                for j in range(TILE)
            }
            inside = (lane >= at) & (lane < at + TILE)
            for t in range(p, count):
                fresh = jnp.where(lane - at == sub, 1.0, 0.0) if t == p else jnp.zeros((TILE, LANES), F32)
                tiles[t][home] = jnp.where(inside, fresh, tiles[t][home])
            for j in range(TILE):

                def row(x, j=j):
                    return jnp.broadcast_to(x[j : j + 1, :], (TILE, LANES))

                scale = lax.rsqrt(row(cols[p, j]))
                pivots = {jj: row(cols[p, jj]) * scale for jj in range(j + 1, TILE)}
                lines = [row(tiles[p][h]) * scale for h in range(lane_tiles)]
                for t in range(p, count):
                    m = cols[t, j] * scale
                    if t == p:
                        m = jnp.where(sub > j, m, 0.0)
                    for jj in range(j + 1, TILE):
                        cols[t, jj] = cols[t, jj] - m * pivots[jj]
                    for h in range(lane_tiles):
                        new = tiles[t][h] - m * lines[h]
                        tiles[t][h] = jnp.where(sub == j, lines[h], new) if t == p else new
        for t in range(count):
            for h in range(lane_tiles):
                work_ref[pl.ds(block + t * TILE, TILE), pl.ds(h * LANES, LANES)] = tiles[t][h]
        end = block + BLOCK
        if end < size:
            done = work_ref[pl.ds(block, BLOCK), :]
            col = lax.broadcasted_iota(jnp.int32, (size, size), 1)
            own_row = lax.broadcasted_iota(jnp.int32, (BLOCK, size), 0) + block
            own_col = lax.broadcasted_iota(jnp.int32, (BLOCK, size), 1)
            change = exact(done, jnp.where((own_col > own_row) & (own_col < end), 0.0, done), TN)
            rest = jnp.where((col >= block) & (col < end), 0.0, work_ref[...])
            rest = rest - change
            work_ref[pl.ds(end, size - end), :] = rest[end:, :]


def factor_kernel(scale, mid_ref, gram_ref, left_ref, project_ref, work_ref):
    peers, height, _ = gram_ref.shape
    rank_width = left_ref.shape[0]
    ranks = mid_ref.shape[0] // peers
    lines = rank_width // ranks // peers
    mid = jnp.concatenate([gathered(mid_ref, peers, lines, r * peers) for r in range(ranks)], axis=0)
    gram_ref = gathered(gram_ref, peers, height * LANES // rank_width)
    half = mid.shape[0] // 2
    upper, lower = mid[:half], mid[half:]
    side = gram_ref[:half, half:]
    corner = jnp.concatenate([gram_ref[half:, :half], gram_ref[half:, half:]], axis=0)
    cross = jnp.concatenate(
        [
            exact(gram_ref[:half, :half], upper, NN) + exact(side, lower, NN),
            exact(side, upper, TN) + exact(corner, lower, NN),
        ],
        axis=0,
    )
    work_ref[...] = exact(mid, cross, TN)
    invert_factor(work_ref)
    row = lax.broadcasted_iota(jnp.int32, work_ref.shape, 0)
    col = lax.broadcasted_iota(jnp.int32, work_ref.shape, 1)
    inverse = jnp.where(row >= col, work_ref[...], 0.0)
    left_ref[...] = exact(mid, inverse, NT) * scale
    project_ref[...] = exact(inverse, cross, NT)


def factored(mid_sum, gram_left, scale, rank_width):
    sketch_width = mid_sum.size // rank_width
    return pl.pallas_call(
        functools.partial(factor_kernel, scale),
        out_shape=(
            jax.ShapeDtypeStruct((rank_width, sketch_width), F32),
            jax.ShapeDtypeStruct((sketch_width, rank_width), F32),
        ),
        scratch_shapes=[pltpu.VMEM((sketch_width, sketch_width), F32)],
        name="factor",
    )(mid_sum, gram_left)


def gram_kernel(rows_ref, out_ref, sum_ref):
    half = rows_ref.shape[1] // 2
    high, low = halves(rows_ref[...])
    first = (high[:, :half], low[:, :half])
    second = (high[:, half:], low[:, half:])
    top = dot3(first, (high, low), TN)
    corner = dot3(second, second, TN)
    corner = jnp.concatenate([corner[: half // 2], corner[half // 2 :]], axis=1)
    total = jnp.concatenate([top, corner], axis=0)
    last = pl.num_programs(0) - 1

    @pl.when(pl.program_id(0) == 0)
    def _():
        sum_ref[...] = total

    @pl.when((pl.program_id(0) > 0) & (pl.program_id(0) < last))
    def _():
        sum_ref[...] += total

    @pl.when(pl.program_id(0) == last)
    def _():
        spread(out_ref, sum_ref[...] + total)


def packed_gram(rows):
    count, depth = rows.shape
    group = 512
    sums = (depth // 2 + depth // 4, depth)
    peers = lax.axis_size(CUTS)
    shape = (peers, sums[0] * sums[1] // LANES // peers, LANES)
    return pl.pallas_call(
        gram_kernel,
        grid=(count // group,),
        in_specs=[pl.BlockSpec((group, depth), lambda g: (g, 0))],
        out_specs=whole_block(shape),
        out_shape=jax.ShapeDtypeStruct(shape, F32),
        scratch_shapes=[pltpu.VMEM(sums, F32)],
        name="gram",
    )(rows)


def apply_kernel(rows_ref, right_ref, out_ref):
    out_ref[...] = dot3(halves(rows_ref[...]), halves(right_ref[...]), NN)


def apply_right(rows, right):
    count, depth = rows.shape
    width = right.shape[1]
    group = 512
    return pl.pallas_call(
        apply_kernel,
        grid=(count // group,),
        in_specs=[pl.BlockSpec((group, depth), lambda g: (g, 0)), whole_block(right.shape)],
        out_specs=pl.BlockSpec((group, width), lambda g: (g, 0)),
        out_shape=jax.ShapeDtypeStruct((count, width), F32),
        name="ortho",
    )(rows, right)


def project_kernel(pieces, rank_ref, project_ref, *refs):
    *stepped_refs, out_ref = refs
    slices = stepped_refs[0].shape[1]
    rows = project_ref.shape[0]
    ranks = len(pieces)
    project = halves(
        jnp.concatenate(
            [project_ref[:, pl.ds(own_block(rank_ref, ranks - distance, ranks), LANES)] for distance in range(ranks)],
            axis=1,
        )
    )
    stepped = [(ref.reshape(-1, LANES), ref.shape[0]) for ref in stepped_refs]
    out = out_ref.reshape(rows * slices, LANES)

    def slab(i):
        return jnp.concatenate([ref[pl.ds(i, count, stride=slices), :] for ref, count in stepped], axis=0)

    for i in range(0, slices, 2):
        product = dot3(project, halves(jnp.concatenate([slab(i), slab(i + 1)], axis=1)), NN)
        for d in range(2):
            out[pl.ds(i + d, rows, stride=slices), :] = product[:, d * LANES : (d + 1) * LANES]


def projected(rank, project, stepped, pieces):
    slices = stepped[0].shape[1]
    rows = project.shape[0]
    return pl.pallas_call(
        functools.partial(project_kernel, pieces),
        grid=(slices // TILE,),
        in_specs=[
            SCALAR,
            whole_block(project.shape),
            *[pl.BlockSpec((block.shape[0], TILE, LANES), lambda g: (0, g, 0)) for block in stepped],
        ],
        out_specs=pl.BlockSpec((rows, TILE, LANES), lambda g: (0, g, 0)),
        out_shape=jax.ShapeDtypeStruct((rows, slices, LANES), F32),
        name="project",
    )(rank, project, *stepped)


def summed(pieces, axes):
    return jnp.sum(lax.all_to_all(pieces, axes, 0, 0, tiled=True), axis=0)


def copies_of(piece, axes):
    copies = jnp.broadcast_to(piece, (lax.axis_size(axes), *piece.shape))
    return lax.all_to_all(copies, axes, 0, 0, tiled=True)


def shifted(array, distance):
    count = lax.axis_size("rank")
    return lax.ppermute(array, "rank", [(i, (i + distance) % count) for i in range(count)])


def neighbours(core):
    count = lax.axis_size(CUTS)
    head, tail = core[:, 0, :], core[:, -1, :]
    below = lax.ppermute(tail, CUTS, [(i, i + 1) for i in range(count - 1)])
    above = lax.ppermute(head, CUTS, [(i + 1, i) for i in range(count - 1)])
    return below, above


def step(core_left, core_mid, core_right, sketch_mid, sketch_right, tail_sketch, stencil):
    row_count, slices, rank_width = core_left.shape
    sketch_width = tail_sketch.shape[1]
    quarters = rank_width // LANES
    ranks = lax.axis_size("rank")
    flat_left = core_left.reshape(row_count * slices, rank_width)

    rank = lax.axis_index("rank").astype(jnp.int32).reshape(1)

    below, above = neighbours(core_mid)
    stepped = step_core(rank, core_mid, below, above, stencil, PIECES)
    own, up, far_up, far_down, down = stepped
    up = shifted(up, 1)
    down = shifted(down, -1)
    far_up = shifted(far_up, 1)
    far_down = shifted(far_down, -1)
    far_up = shifted(far_up, 1)
    far_down = shifted(far_down, -1)

    gram_left = packed_gram(flat_left)
    gram_left = summed(gram_left, CUTS)
    gram_left = sum([shifted(gram_left, d) for d in range(1, ranks)], gram_left)
    gram_left = copies_of(gram_left, CUTS)

    right_part = contract_back(rank, [core_right], (), tail_sketch, sketch_right)
    right_sum = summed(right_part, CUTS)
    right_sum = copies_of(right_sum, EVERY)

    mid_part = contract_back(rank, stepped, PIECES, right_sum, sketch_mid)
    mid_sum = summed(mid_part, CUTS)
    mid_sum = copies_of(mid_sum, EVERY)

    scale = math.sqrt(rank_width * slices * lax.axis_size(CUTS))
    left, project = factored(mid_sum, gram_left, scale, rank_width)
    product = projected(rank, project, [own, up, far_up, far_down, down], PIECES)
    blocks = product.reshape(ranks, sketch_width // ranks, slices, LANES)
    arrived = lax.all_to_all(blocks, "rank", 0, 0, tiled=True)
    next_core = jnp.moveaxis(arrived, 0, 2).reshape(sketch_width // ranks, slices, quarters * LANES)
    ortho_core = apply_right(flat_left, left).reshape(row_count, slices, sketch_width)
    return ortho_core, next_core


def solution(mesh):
    split = Mesh(
        mesh.devices.reshape(4, 4, 2, mesh.shape["rank"]), ("cuts_0", "cuts_1", "cuts_2", "rank")
    )
    in_specs = (
        P("rank", CUTS, None),
        P("rank", CUTS, None),
        P("rank", CUTS, None),
        P(None, CUTS, None),
        P(None, CUTS, None),
        P(),
        P(None, CUTS),
    )
    out_specs = (P("rank", CUTS, None), P("rank", CUTS, None))
    return jax.shard_map(step, mesh=split, in_specs=in_specs, out_specs=out_specs, check_vma=False)
```

```python
import functools
import math

import jax
import jax.numpy as jnp
from jax import lax
from jax.experimental import pallas as pl
from jax.experimental.pallas import tpu as pltpu
from jax.sharding import Mesh
from jax.sharding import PartitionSpec as P

CUTS = ("cuts_0", "cuts_1", "cuts_2")
EVERY = ("rank", "cuts_0", "cuts_1", "cuts_2")
HIGHEST = lax.Precision.HIGHEST
F32 = jnp.float32
BF16 = jnp.bfloat16
LANES = 128
TILE = 8
BLOCK = 64
PIECES = (1, 1, 2, 1)
STEPS = 4
SKETCH_STEPS = 2
GROUP = 16

NN = (((1,), (0,)), ((), ()))
NT = (((1,), (1,)), ((), ()))
TN = (((0,), (0,)), ((), ()))


def halves(x):
    high = x.astype(BF16)
    return high, (x - high.astype(F32)).astype(BF16)


def dot3(a, b, dims):
    (ah, al), (bh, bl) = a, b
    dot = functools.partial(lax.dot_general, dimension_numbers=dims, preferred_element_type=F32)
    return dot(ah, bh) + (dot(ah, bl) + dot(al, bh))


def exact(a, b, dims):
    return lax.dot_general(a, b, dims, precision=HIGHEST, preferred_element_type=F32)


def whole_block(shape):
    return pl.BlockSpec(shape, lambda *_: (0,) * len(shape))


def own_block(rank_ref, distance, ranks):
    return pl.multiple_of(lax.rem(rank_ref[0] + distance, ranks) * LANES, LANES)


def spread(out_ref, total):
    peers, height, _ = out_ref.shape
    out = out_ref.reshape(peers * height, LANES)
    lines = total.shape[0] // peers
    for h in range(total.shape[1] // LANES):
        for j in range(lines):
            block = total[j * peers : (j + 1) * peers, h * LANES : (h + 1) * LANES]
            out[pl.ds(h * lines + j, peers, stride=height), :] = block


def gathered(ref, peers, lines, first=0):
    count, height, _ = ref.shape
    flat = ref.reshape(count * height, LANES)
    return jnp.concatenate(
        [
            jnp.concatenate(
                [flat[pl.ds(first * height + h * lines + j, peers, stride=height), :] for h in range(height // lines)],
                axis=1,
            )
            for j in range(lines)
        ],
        axis=0,
    )


def started(source, target, sem):
    copy = pltpu.make_async_copy(source, target, sem)
    copy.start()
    return copy


def contract_kernel(core_parts, rank_ref, part_ref, *refs):
    count = sum(core_parts) if core_parts else 1
    core_hbm, sketch_hbm, out_ref, *refs = refs[:count], refs[count], refs[count + 1], *refs[count + 2 :]
    core_refs, (sketch_ref, applied_ref, core_sems, sketch_sems) = refs[:count], refs[count:]
    peers = out_ref.shape[0]
    slices = core_refs[0].shape[1]
    rows = core_refs[0].shape[0]
    pieces, sketch_rows = sketch_ref.shape[:2]
    step = rows // STEPS

    plan = []
    for k in range(STEPS):
        at = 0
        for split in core_parts or (1,):
            n, begin = divmod(k * step, rows // split)
            plan.append((k, at + n, pl.ds(begin, step)))
            at += split
    arriving = [
        (k, index, lines, started(core_hbm[index].at[lines], core_refs[index].at[lines], core_sems.at[n]))
        for n, (k, index, lines) in enumerate(plan)
    ]
    sketch_part = sketch_rows // SKETCH_STEPS
    sketches_arriving = []
    for c in range(SKETCH_STEPS):
        lines = pl.ds(c * sketch_part, sketch_part)
        for h in range(pieces):
            source = sketch_hbm.at[lines, :, pl.ds(h * LANES, LANES)]
            sketches_arriving.append(started(source, sketch_ref.at[h, lines], sketch_sems.at[c * pieces + h]))

    if core_parts:
        blocks = [lax.rem(rank_ref[0] + distance, len(core_parts)) for distance in range(len(core_parts))]
        part = jnp.concatenate([gathered(part_ref, peers, LANES // peers, block * peers) for block in blocks], axis=0)
    else:
        part = part_ref[...]
    part = halves(part)
    for k in range(STEPS):
        taken = []
        for chunk, index, lines, copy in arriving:
            if chunk == k:
                copy.wait()
                taken.append(core_refs[index][lines].reshape(step * slices, -1))
        core = taken[0] if len(taken) == 1 else jnp.concatenate(taken, axis=1)
        applied = dot3(halves(core), part, NN)
        for h in range(pieces):
            applied_ref[h, pl.ds(k * step * slices, step * slices), :] = applied[:, h * LANES : (h + 1) * LANES]
    for copy in sketches_arriving:
        copy.wait()
    sketches = [sketch_ref.at[h].reshape(sketch_rows * slices, LANES) for h in range(pieces)]

    def run(g, total):
        for i in range(TILE):
            at = g * TILE + i
            left = [applied_ref.at[h][pl.ds(at, rows, stride=slices), :] for h in range(pieces)]
            right = [ref[pl.ds(at, sketch_rows, stride=slices), :] for ref in sketches]
            total += dot3(halves(jnp.concatenate(left, axis=1)), halves(jnp.concatenate(right, axis=1)), NT)
        return total

    total = lax.fori_loop(0, slices // TILE, run, jnp.zeros((rows, sketch_rows), F32))
    spread(out_ref, total)


SCALAR = pl.BlockSpec(memory_space=pltpu.SMEM)
IN_VMEM = pl.BlockSpec(memory_space=pltpu.VMEM)
IN_HBM = pl.BlockSpec(memory_space=pltpu.HBM)


def contract_back(rank, cores, core_parts, part, sketch):
    rows, slices = cores[0].shape[:2]
    sketch_rows, _, sketch_cols = sketch.shape
    pieces = sketch_cols // LANES
    peers = lax.axis_size(CUTS)
    shape = (peers, rows * sketch_rows // LANES // peers, LANES)
    return pl.pallas_call(
        functools.partial(contract_kernel, core_parts),
        in_specs=[SCALAR, IN_VMEM, *[IN_HBM] * (len(cores) + 1)],
        out_specs=IN_VMEM,
        out_shape=jax.ShapeDtypeStruct(shape, F32),
        scratch_shapes=[
            *[pltpu.VMEM(core.shape, F32) for core in cores],
            pltpu.VMEM((pieces, sketch_rows, slices, LANES), F32),
            pltpu.VMEM((pieces, rows * slices, LANES), F32),
            pltpu.SemaphoreType.DMA((STEPS * max(1, len(core_parts)),)),
            pltpu.SemaphoreType.DMA((SKETCH_STEPS * pieces,)),
        ],
        name="contract",
    )(rank, part, *cores, sketch)


def stencil_kernel(pieces, rank_ref, core_hbm, below_ref, above_ref, coef_ref, *refs):
    count = sum(pieces)
    outs_hbm, core_all, step_refs, (in_sems, out_sems) = refs[:count], refs[count], refs[count + 1 : -2], refs[-2:]
    total, slices, _ = core_all.shape
    rows = GROUP
    groups = total // rows
    lines = [pl.ds(g * rows, rows) for g in range(groups)]
    arriving = [started(core_hbm.at[lines[g]], core_all.at[lines[g]], in_sems.at[g]) for g in range(groups)]
    place = lax.broadcasted_iota(jnp.int32, (rows * slices, LANES), 0) % slices
    coef = [jnp.broadcast_to(coef_ref[k][None], (rows, slices, LANES)).reshape(rows * slices, LANES) for k in range(3)]
    leaving = []
    for g in range(groups):
        arriving[g].wait()
        at = 0
        for distance, split in enumerate(pieces):
            cols = pl.ds(own_block(rank_ref, distance, len(pieces)), LANES)
            core = core_all[lines[g], :, cols].reshape(rows * slices, LANES)
            first = jnp.broadcast_to(below_ref[lines[g], cols][:, None, :], (rows, slices, LANES))
            last = jnp.broadcast_to(above_ref[lines[g], cols][:, None, :], (rows, slices, LANES))
            below = jnp.where(place == 0, first.reshape(rows * slices, LANES), pltpu.roll(core, 1, 0))
            above = jnp.where(
                place == slices - 1, last.reshape(rows * slices, LANES), pltpu.roll(core, rows * slices - 1, 0)
            )
            stepped = (coef[0] * below + coef[1] * core + coef[2] * above).reshape(rows, slices, LANES)
            n, begin = divmod(g * rows, total // split)
            target = pl.ds(begin, rows)
            step_refs[at + n][target] = stepped
            sem = out_sems.at[g * len(pieces) + distance]
            leaving.append(started(step_refs[at + n].at[target], outs_hbm[at + n].at[target], sem))
            at += split
    for copy in leaving:
        copy.wait()


def step_core(rank, core, below, above, stencil, pieces):
    rows, slices, _ = core.shape
    coef = jnp.broadcast_to(stencil[:, :, None], (3, slices, LANES))
    shapes = [(rows // split, slices, LANES) for split in pieces for _ in range(split)]
    return pl.pallas_call(
        functools.partial(stencil_kernel, pieces),
        in_specs=[SCALAR, IN_HBM, IN_VMEM, IN_VMEM, IN_VMEM],
        out_specs=[IN_HBM] * len(shapes),
        out_shape=[jax.ShapeDtypeStruct(shape, F32) for shape in shapes],
        scratch_shapes=[
            pltpu.VMEM(core.shape, F32),
            *[pltpu.VMEM(shape, F32) for shape in shapes],
            pltpu.SemaphoreType.DMA((rows // GROUP,)),
            pltpu.SemaphoreType.DMA((rows // GROUP * len(pieces),)),
        ],
        name="stencil",
    )(rank, core, below, above, coef)


def invert_factor(work_ref):
    size = work_ref.shape[0]
    lane_tiles = size // LANES
    sub = lax.broadcasted_iota(jnp.int32, (TILE, LANES), 0)
    lane = lax.broadcasted_iota(jnp.int32, (TILE, LANES), 1)
    for block in range(0, size, BLOCK):
        count = BLOCK // TILE
        tiles = [
            [work_ref[pl.ds(block + t * TILE, TILE), pl.ds(h * LANES, LANES)] for h in range(lane_tiles)]
            for t in range(count)
        ]
        for p in range(count):
            k = block + p * TILE
            home, at = divmod(k, LANES)
            cols = {
                (t, j): jnp.broadcast_to(tiles[t][home][:, at + j : at + j + 1], (TILE, LANES))
                for t in range(p, count)
                for j in range(TILE)
            }
            inside = (lane >= at) & (lane < at + TILE)
            for t in range(p, count):
                fresh = jnp.where(lane - at == sub, 1.0, 0.0) if t == p else jnp.zeros((TILE, LANES), F32)
                tiles[t][home] = jnp.where(inside, fresh, tiles[t][home])
            for j in range(TILE):

                def row(x, j=j):
                    return jnp.broadcast_to(x[j : j + 1, :], (TILE, LANES))

                scale = lax.rsqrt(row(cols[p, j]))
                pivots = {jj: row(cols[p, jj]) * scale for jj in range(j + 1, TILE)}
                lines = [row(tiles[p][h]) * scale for h in range(lane_tiles)]
                for t in range(p, count):
                    m = cols[t, j] * scale
                    if t == p:
                        m = jnp.where(sub > j, m, 0.0)
                    for jj in range(j + 1, TILE):
                        cols[t, jj] = cols[t, jj] - m * pivots[jj]
                    for h in range(lane_tiles):
                        new = tiles[t][h] - m * lines[h]
                        tiles[t][h] = jnp.where(sub == j, lines[h], new) if t == p else new
        for t in range(count):
            for h in range(lane_tiles):
                work_ref[pl.ds(block + t * TILE, TILE), pl.ds(h * LANES, LANES)] = tiles[t][h]
        end = block + BLOCK
        if end < size:
            done = work_ref[pl.ds(block, BLOCK), :]
            col = lax.broadcasted_iota(jnp.int32, (size, size), 1)
            own_row = lax.broadcasted_iota(jnp.int32, (BLOCK, size), 0) + block
            own_col = lax.broadcasted_iota(jnp.int32, (BLOCK, size), 1)
            change = exact(done, jnp.where((own_col > own_row) & (own_col < end), 0.0, done), TN)
            rest = jnp.where((col >= block) & (col < end), 0.0, work_ref[...])
            rest = rest - change
            work_ref[pl.ds(end, size - end), :] = rest[end:, :]


def factor_kernel(scale, mid_ref, gram_ref, left_ref, project_ref, work_ref):
    peers, height, _ = gram_ref.shape
    rank_width = left_ref.shape[0]
    ranks = mid_ref.shape[0] // peers
    lines = rank_width // ranks // peers
    mid = jnp.concatenate([gathered(mid_ref, peers, lines, r * peers) for r in range(ranks)], axis=0)
    gram_ref = gathered(gram_ref, peers, height * LANES // rank_width)
    half = mid.shape[0] // 2
    upper, lower = mid[:half], mid[half:]
    side = gram_ref[:half, half:]
    corner = jnp.concatenate([gram_ref[half:, :half], gram_ref[half:, half:]], axis=0)
    cross = jnp.concatenate(
        [
            exact(gram_ref[:half, :half], upper, NN) + exact(side, lower, NN),
            exact(side, upper, TN) + exact(corner, lower, NN),
        ],
        axis=0,
    )
    work_ref[...] = exact(mid, cross, TN)
    invert_factor(work_ref)
    row = lax.broadcasted_iota(jnp.int32, work_ref.shape, 0)
    col = lax.broadcasted_iota(jnp.int32, work_ref.shape, 1)
    inverse = jnp.where(row >= col, work_ref[...], 0.0)
    left_ref[...] = exact(mid, inverse, NT) * scale
    project_ref[...] = exact(inverse, cross, NT)


def factored(mid_sum, gram_left, scale, rank_width):
    sketch_width = mid_sum.size // rank_width
    return pl.pallas_call(
        functools.partial(factor_kernel, scale),
        out_shape=(
            jax.ShapeDtypeStruct((rank_width, sketch_width), F32),
            jax.ShapeDtypeStruct((sketch_width, rank_width), F32),
        ),
        scratch_shapes=[pltpu.VMEM((sketch_width, sketch_width), F32)],
        name="factor",
    )(mid_sum, gram_left)


def gram_kernel(rows_hbm, out_ref, rows_ref, sum_ref, sems):
    count, depth = rows_ref.shape
    half = depth // 2
    part = count // STEPS

    def copy_of(k):
        lines = pl.ds(pl.multiple_of(k * part, part), part)
        return lines, pltpu.make_async_copy(rows_hbm.at[lines], rows_ref.at[lines], sems.at[k])

    for k in range(STEPS):
        copy_of(k)[1].start()
    sum_ref[...] = jnp.zeros_like(sum_ref)

    def run(k, carry):
        lines, copy = copy_of(k)
        copy.wait()
        high, low = halves(rows_ref[lines, :])
        first = (high[:, :half], low[:, :half])
        second = (high[:, half:], low[:, half:])
        sum_ref[:half, :] += dot3(first, (high, low), TN)
        corner = dot3(second, second, TN)
        sum_ref[half:, :half] += corner[: half // 2]
        sum_ref[half:, half:] += corner[half // 2 :]
        return carry

    lax.fori_loop(0, STEPS, run, 0)
    spread(out_ref, sum_ref[...])


def packed_gram(rows):
    depth = rows.shape[1]
    sums = (depth // 2 + depth // 4, depth)
    peers = lax.axis_size(CUTS)
    shape = (peers, sums[0] * sums[1] // LANES // peers, LANES)
    return pl.pallas_call(
        gram_kernel,
        in_specs=[IN_HBM],
        out_specs=IN_VMEM,
        out_shape=jax.ShapeDtypeStruct(shape, F32),
        scratch_shapes=[pltpu.VMEM(rows.shape, F32), pltpu.VMEM(sums, F32), pltpu.SemaphoreType.DMA((STEPS,))],
        name="gram",
    )(rows)


def apply_kernel(rows_ref, right_ref, out_ref):
    out_ref[...] = dot3(halves(rows_ref[...]), halves(right_ref[...]), NN)


def apply_right(rows, right):
    count, depth = rows.shape
    width = right.shape[1]
    group = 512
    return pl.pallas_call(
        apply_kernel,
        grid=(count // group,),
        in_specs=[pl.BlockSpec((group, depth), lambda g: (g, 0)), whole_block(right.shape)],
        out_specs=pl.BlockSpec((group, width), lambda g: (g, 0)),
        out_shape=jax.ShapeDtypeStruct((count, width), F32),
        name="ortho",
    )(rows, right)


def project_kernel(pieces, rank_ref, project_ref, *refs):
    count = sum(pieces)
    blocks_hbm, out_hbm, block_refs, (out_ref, in_sems, out_sems) = refs[:count], refs[count], refs[count + 1 : -3], refs[-3:]
    slices = blocks_hbm[0].shape[1]
    rows = project_ref.shape[0]
    ranks = len(pieces)
    groups = slices // TILE
    slabs = [pl.ds(g * TILE, TILE) for g in range(groups)]
    arriving = [
        [started(hbm.at[:, slabs[g]], ref.at[g], in_sems.at[g * count + n]) for n, (hbm, ref) in enumerate(zip(blocks_hbm, block_refs))]
        for g in range(groups)
    ]
    project = halves(
        jnp.concatenate(
            [project_ref[:, pl.ds(own_block(rank_ref, ranks - distance, ranks), LANES)] for distance in range(ranks)],
            axis=1,
        )
    )
    leaving = []
    for g in range(groups):
        for copy in arriving[g]:
            copy.wait()
        stepped = [(ref.at[g].reshape(-1, LANES), ref.shape[1]) for ref in block_refs]
        out = out_ref.at[g].reshape(rows * TILE, LANES)

        def slab(i, stepped=stepped):
            return jnp.concatenate([ref[pl.ds(i, length, stride=TILE), :] for ref, length in stepped], axis=0)

        for i in range(0, TILE, 2):
            product = dot3(project, halves(jnp.concatenate([slab(i), slab(i + 1)], axis=1)), NN)
            for d in range(2):
                out[pl.ds(i + d, rows, stride=TILE), :] = product[:, d * LANES : (d + 1) * LANES]
        leaving.append(started(out_ref.at[g], out_hbm.at[:, slabs[g]], out_sems.at[g]))
    for copy in leaving:
        copy.wait()


def projected(rank, project, stepped, pieces):
    slices = stepped[0].shape[1]
    rows = project.shape[0]
    groups = slices // TILE
    return pl.pallas_call(
        functools.partial(project_kernel, pieces),
        in_specs=[SCALAR, IN_VMEM, *[IN_HBM] * len(stepped)],
        out_specs=IN_HBM,
        out_shape=jax.ShapeDtypeStruct((rows, slices, LANES), F32),
        scratch_shapes=[
            *[pltpu.VMEM((groups, block.shape[0], TILE, LANES), F32) for block in stepped],
            pltpu.VMEM((groups, rows, TILE, LANES), F32),
            pltpu.SemaphoreType.DMA((groups * len(stepped),)),
            pltpu.SemaphoreType.DMA((groups,)),
        ],
        name="project",
    )(rank, project, *stepped)


def summed(pieces, axes):
    return jnp.sum(lax.all_to_all(pieces, axes, 0, 0, tiled=True), axis=0)


def copies_of(piece, axes):
    copies = jnp.broadcast_to(piece, (lax.axis_size(axes), *piece.shape))
    return lax.all_to_all(copies, axes, 0, 0, tiled=True)


def shifted(array, distance):
    count = lax.axis_size("rank")
    return lax.ppermute(array, "rank", [(i, (i + distance) % count) for i in range(count)])


def neighbours(core):
    count = lax.axis_size(CUTS)
    head, tail = core[:, 0, :], core[:, -1, :]
    below = lax.ppermute(tail, CUTS, [(i, i + 1) for i in range(count - 1)])
    above = lax.ppermute(head, CUTS, [(i + 1, i) for i in range(count - 1)])
    return below, above


def step(core_left, core_mid, core_right, sketch_mid, sketch_right, tail_sketch, stencil):
    row_count, slices, rank_width = core_left.shape
    sketch_width = tail_sketch.shape[1]
    quarters = rank_width // LANES
    ranks = lax.axis_size("rank")
    flat_left = core_left.reshape(row_count * slices, rank_width)

    rank = lax.axis_index("rank").astype(jnp.int32).reshape(1)

    below, above = neighbours(core_mid)
    stepped = step_core(rank, core_mid, below, above, stencil, PIECES)
    own, up, far_up, far_down, down = stepped
    up = shifted(up, 1)
    down = shifted(down, -1)
    far_up = shifted(far_up, 1)
    far_down = shifted(far_down, -1)
    far_up = shifted(far_up, 1)
    far_down = shifted(far_down, -1)

    gram_left = packed_gram(flat_left)
    gram_left = summed(gram_left, CUTS)
    gram_left = sum([shifted(gram_left, d) for d in range(1, ranks)], gram_left)
    gram_left = copies_of(gram_left, CUTS)

    right_part = contract_back(rank, [core_right], (), tail_sketch, sketch_right)
    right_sum = summed(right_part, CUTS)
    right_sum = copies_of(right_sum, EVERY)

    mid_part = contract_back(rank, stepped, PIECES, right_sum, sketch_mid)
    mid_sum = summed(mid_part, CUTS)
    mid_sum = copies_of(mid_sum, EVERY)

    scale = math.sqrt(rank_width * slices * lax.axis_size(CUTS))
    left, project = factored(mid_sum, gram_left, scale, rank_width)
    product = projected(rank, project, [own, up, far_up, far_down, down], PIECES)
    blocks = product.reshape(ranks, sketch_width // ranks, slices, LANES)
    arrived = lax.all_to_all(blocks, "rank", 0, 0, tiled=True)
    next_core = jnp.moveaxis(arrived, 0, 2).reshape(sketch_width // ranks, slices, quarters * LANES)
    ortho_core = apply_right(flat_left, left).reshape(row_count, slices, sketch_width)
    return ortho_core, next_core


def solution(mesh):
    split = Mesh(
        mesh.devices.reshape(4, 4, 2, mesh.shape["rank"]), ("cuts_0", "cuts_1", "cuts_2", "rank")
    )
    in_specs = (
        P("rank", CUTS, None),
        P("rank", CUTS, None),
        P("rank", CUTS, None),
        P(None, CUTS, None),
        P(None, CUTS, None),
        P(),
        P(None, CUTS),
    )
    out_specs = (P("rank", CUTS, None), P("rank", CUTS, None))
    return jax.shard_map(step, mesh=split, in_specs=in_specs, out_specs=out_specs, check_vma=False)
```

```python
import functools
import math

import jax
import jax.numpy as jnp
from jax import lax
from jax.experimental import pallas as pl
from jax.experimental.pallas import tpu as pltpu
from jax.sharding import Mesh
from jax.sharding import PartitionSpec as P

CUTS = ("cuts_0", "cuts_1", "cuts_2")
EVERY = ("rank", "cuts_0", "cuts_1", "cuts_2")
HIGHEST = lax.Precision.HIGHEST
F32 = jnp.float32
BF16 = jnp.bfloat16
LANES = 128
TILE = 8
BLOCK = 64
PIECES = (1, 1, 2, 1)
STEPS = 4

NN = (((1,), (0,)), ((), ()))
NT = (((1,), (1,)), ((), ()))
TN = (((0,), (0,)), ((), ()))


def halves(x):
    high = x.astype(BF16)
    return high, (x - high.astype(F32)).astype(BF16)


def dot3(a, b, dims):
    (ah, al), (bh, bl) = a, b
    dot = functools.partial(lax.dot_general, dimension_numbers=dims, preferred_element_type=F32)
    return dot(ah, bh) + (dot(ah, bl) + dot(al, bh))


def exact(a, b, dims):
    return lax.dot_general(a, b, dims, precision=HIGHEST, preferred_element_type=F32)


def whole_block(shape):
    return pl.BlockSpec(shape, lambda *_: (0,) * len(shape))


def own_block(rank_ref, distance, ranks):
    return pl.multiple_of(lax.rem(rank_ref[0] + distance, ranks) * LANES, LANES)


def spread(out_ref, total):
    peers, height, _ = out_ref.shape
    out = out_ref.reshape(peers * height, LANES)
    lines = total.shape[0] // peers
    for h in range(total.shape[1] // LANES):
        for j in range(lines):
            block = total[j * peers : (j + 1) * peers, h * LANES : (h + 1) * LANES]
            out[pl.ds(h * lines + j, peers, stride=height), :] = block


def gathered(ref, peers, lines, first=0):
    count, height, _ = ref.shape
    flat = ref.reshape(count * height, LANES)
    return jnp.concatenate(
        [
            jnp.concatenate(
                [flat[pl.ds(first * height + h * lines + j, peers, stride=height), :] for h in range(height // lines)],
                axis=1,
            )
            for j in range(lines)
        ],
        axis=0,
    )


def started(source, target, sem):
    copy = pltpu.make_async_copy(source, target, sem)
    copy.start()
    return copy


def contract_kernel(core_parts, rank_ref, part_ref, *refs):
    count = sum(core_parts) if core_parts else 1
    core_hbm, sketch_hbm, out_ref, *refs = refs[:count], refs[count], refs[count + 1], *refs[count + 2 :]
    core_refs, (sketch_ref, applied_ref, core_sems, sketch_sems) = refs[:count], refs[count:]
    peers = out_ref.shape[0]
    pieces, groups, sketch_rows = sketch_ref.shape[:3]
    slices = groups * TILE
    rows = applied_ref.shape[1] // slices
    step = core_refs[0].shape[0] // STEPS

    arriving = []
    for k in range(STEPS):
        lines = pl.ds(k * step, step)
        for n, (hbm, ref) in enumerate(zip(core_hbm, core_refs)):
            arriving.append((k, started(hbm.at[lines], ref.at[lines], core_sems.at[k * count + n])))
    sketches_arriving = [
        started(
            sketch_hbm.at[:, pl.ds(g * TILE, TILE), pl.ds(h * LANES, LANES)],
            sketch_ref.at[h, g],
            sketch_sems.at[g * pieces + h],
        )
        for g in range(groups)
        for h in range(pieces)
    ]

    if core_parts:
        blocks = [lax.rem(rank_ref[0] + distance, len(core_parts)) for distance in range(len(core_parts))]
        part = jnp.concatenate([gathered(part_ref, peers, LANES // peers, block * peers) for block in blocks], axis=0)
    else:
        part = part_ref[...]
    part = halves(part)
    for k in range(STEPS):
        for chunk, copy in arriving:
            if chunk == k:
                copy.wait()
        if core_parts:
            slabs = []
            for i in range(k * step, (k + 1) * step):
                taken, blocks = list(core_refs), []
                for split in core_parts:
                    block = [taken.pop(0)[i] for _ in range(split)]
                    blocks.append(block[0] if split == 1 else jnp.concatenate(block, axis=0))
                slabs.append(jnp.concatenate(blocks, axis=1))
            core = jnp.concatenate(slabs, axis=0)
        else:
            core = core_refs[0][pl.ds(k * step, step)].reshape(step * slices, -1)
        applied = dot3(halves(core), part, NN)
        for h in range(pieces):
            own = applied[:, h * LANES : (h + 1) * LANES]
            if core_parts:
                applied_ref[h, pl.ds(k * step * rows, step * rows), :] = own
                continue
            own = own.reshape(step, groups, TILE, LANES)
            for g in range(groups):
                begin = (g * rows + k * step) * TILE
                applied_ref[h, pl.ds(begin, step * TILE), :] = own[:, g].reshape(step * TILE, LANES)
    for copy in sketches_arriving:
        copy.wait()

    def run(g, total):
        for i in range(TILE):
            if core_parts:
                lines = pl.ds(pl.multiple_of((g * TILE + i) * rows, rows), rows)
            else:
                lines = pl.ds(g * rows * TILE + i, rows, stride=TILE)
            left = [applied_ref.at[h][lines, :] for h in range(pieces)]
            right = [
                sketch_ref.at[h, g].reshape(sketch_rows * TILE, LANES)[pl.ds(i, sketch_rows, stride=TILE), :]
                for h in range(pieces)
            ]
            total += dot3(halves(jnp.concatenate(left, axis=1)), halves(jnp.concatenate(right, axis=1)), NT)
        return total

    spread(out_ref, lax.fori_loop(0, groups, run, jnp.zeros((rows, sketch_rows), F32)))


SCALAR = pl.BlockSpec(memory_space=pltpu.SMEM)
IN_VMEM = pl.BlockSpec(memory_space=pltpu.VMEM)
IN_HBM = pl.BlockSpec(memory_space=pltpu.HBM)


def contract_back(rank, cores, core_parts, part, sketch):
    sketch_rows, slices, sketch_cols = sketch.shape
    rows = cores[0].shape[1 if core_parts else 0]
    pieces = sketch_cols // LANES
    peers = lax.axis_size(CUTS)
    shape = (peers, rows * sketch_rows // LANES // peers, LANES)
    return pl.pallas_call(
        functools.partial(contract_kernel, core_parts),
        in_specs=[SCALAR, IN_VMEM, *[IN_HBM] * (len(cores) + 1)],
        out_specs=IN_VMEM,
        out_shape=jax.ShapeDtypeStruct(shape, F32),
        scratch_shapes=[
            *[pltpu.VMEM(core.shape, F32) for core in cores],
            pltpu.VMEM((pieces, slices // TILE, sketch_rows, TILE, LANES), F32),
            pltpu.VMEM((pieces, rows * slices, LANES), F32),
            pltpu.SemaphoreType.DMA((STEPS * len(cores),)),
            pltpu.SemaphoreType.DMA((pieces * slices // TILE,)),
        ],
        name="contract",
    )(rank, part, *cores, sketch)


def stencil_kernel(pieces, rank_ref, coef_ref, core_hbm, below_ref, above_ref, *refs):
    count = sum(pieces)
    outs_hbm, core_ref, step_refs, (in_sems, out_sems) = refs[:count], refs[count], refs[count + 1 : -2], refs[-2:]
    groups, blocks, rows, _, _ = core_ref.shape
    slices = groups * TILE
    arriving = [
        [
            started(
                core_hbm.at[:, pl.ds(g * TILE, TILE), pl.ds(own_block(rank_ref, distance, blocks), LANES)],
                core_ref.at[g, distance],
                in_sems.at[g * blocks + distance],
            )
            for g in range(groups)
        ]
        for distance in range(blocks)
    ]
    leaving, at = [], 0
    for distance, split in enumerate(pieces):
        for copy in arriving[distance]:
            copy.wait()
        cols = pl.ds(own_block(rank_ref, distance, blocks), LANES)

        def slab(i, distance=distance, cols=cols):
            if i < 0:
                return below_ref[:, cols]
            if i == slices:
                return above_ref[:, cols]
            flat = core_ref.at[i // TILE, distance].reshape(rows * TILE, LANES)
            return flat[pl.ds(i % TILE, rows, stride=TILE), :]

        below, core = slab(-1), slab(0)
        part = rows // split
        for i in range(slices):
            above = slab(i + 1)
            stepped = coef_ref[0, i] * below + coef_ref[1, i] * core + coef_ref[2, i] * above
            for n in range(split):
                step_refs[at + n][i] = stepped[n * part : (n + 1) * part]
            below, core = core, above
        for n in range(split):
            leaving.append(started(step_refs[at + n], outs_hbm[at + n], out_sems.at[at + n]))
        at += split
    for copy in leaving:
        copy.wait()


def step_core(rank, core, below, above, stencil, pieces):
    rows, slices, _ = core.shape
    groups, blocks = slices // TILE, len(pieces)
    shapes = [(slices, rows // split, LANES) for split in pieces for _ in range(split)]
    return pl.pallas_call(
        functools.partial(stencil_kernel, pieces),
        in_specs=[SCALAR, SCALAR, IN_HBM, IN_VMEM, IN_VMEM],
        out_specs=[IN_HBM] * len(shapes),
        out_shape=[jax.ShapeDtypeStruct(shape, F32) for shape in shapes],
        scratch_shapes=[
            pltpu.VMEM((groups, blocks, rows, TILE, LANES), F32),
            *[pltpu.VMEM(shape, F32) for shape in shapes],
            pltpu.SemaphoreType.DMA((groups * blocks,)),
            pltpu.SemaphoreType.DMA((len(shapes),)),
        ],
        name="stencil",
    )(rank, stencil, core, below, above)


def invert_factor(work_ref):
    size = work_ref.shape[0]
    lane_tiles = size // LANES
    sub = lax.broadcasted_iota(jnp.int32, (TILE, LANES), 0)
    lane = lax.broadcasted_iota(jnp.int32, (TILE, LANES), 1)
    for block in range(0, size, BLOCK):
        count = BLOCK // TILE
        tiles = [
            [work_ref[pl.ds(block + t * TILE, TILE), pl.ds(h * LANES, LANES)] for h in range(lane_tiles)]
            for t in range(count)
        ]
        for p in range(count):
            k = block + p * TILE
            home, at = divmod(k, LANES)
            cols = {
                (t, j): jnp.broadcast_to(tiles[t][home][:, at + j : at + j + 1], (TILE, LANES))
                for t in range(p, count)
                for j in range(TILE)
            }
            inside = (lane >= at) & (lane < at + TILE)
            for t in range(p, count):
                fresh = jnp.where(lane - at == sub, 1.0, 0.0) if t == p else jnp.zeros((TILE, LANES), F32)
                tiles[t][home] = jnp.where(inside, fresh, tiles[t][home])
            for j in range(TILE):

                def row(x, j=j):
                    return jnp.broadcast_to(x[j : j + 1, :], (TILE, LANES))

                scale = lax.rsqrt(row(cols[p, j]))
                pivots = {jj: row(cols[p, jj]) * scale for jj in range(j + 1, TILE)}
                lines = [row(tiles[p][h]) * scale for h in range(lane_tiles)]
                for t in range(p, count):
                    m = cols[t, j] * scale
                    if t == p:
                        m = jnp.where(sub > j, m, 0.0)
                    for jj in range(j + 1, TILE):
                        cols[t, jj] = cols[t, jj] - m * pivots[jj]
                    for h in range(lane_tiles):
                        new = tiles[t][h] - m * lines[h]
                        tiles[t][h] = jnp.where(sub == j, lines[h], new) if t == p else new
        for t in range(count):
            for h in range(lane_tiles):
                work_ref[pl.ds(block + t * TILE, TILE), pl.ds(h * LANES, LANES)] = tiles[t][h]
        end = block + BLOCK
        if end < size:
            done = work_ref[pl.ds(block, BLOCK), :]
            col = lax.broadcasted_iota(jnp.int32, (size, size), 1)
            own_row = lax.broadcasted_iota(jnp.int32, (BLOCK, size), 0) + block
            own_col = lax.broadcasted_iota(jnp.int32, (BLOCK, size), 1)
            change = exact(done, jnp.where((own_col > own_row) & (own_col < end), 0.0, done), TN)
            rest = jnp.where((col >= block) & (col < end), 0.0, work_ref[...])
            rest = rest - change
            work_ref[pl.ds(end, size - end), :] = rest[end:, :]


def factor_kernel(scale, mid_ref, gram_ref, left_ref, project_ref, work_ref):
    peers, height, _ = gram_ref.shape
    rank_width = left_ref.shape[0]
    ranks = mid_ref.shape[0] // peers
    lines = rank_width // ranks // peers
    mid = jnp.concatenate([gathered(mid_ref, peers, lines, r * peers) for r in range(ranks)], axis=0)
    gram_ref = gathered(gram_ref, peers, height * LANES // rank_width)
    half = mid.shape[0] // 2
    upper, lower = mid[:half], mid[half:]
    side = gram_ref[:half, half:]
    corner = jnp.concatenate([gram_ref[half:, :half], gram_ref[half:, half:]], axis=0)
    cross = jnp.concatenate(
        [
            exact(gram_ref[:half, :half], upper, NN) + exact(side, lower, NN),
            exact(side, upper, TN) + exact(corner, lower, NN),
        ],
        axis=0,
    )
    work_ref[...] = exact(mid, cross, TN)
    invert_factor(work_ref)
    row = lax.broadcasted_iota(jnp.int32, work_ref.shape, 0)
    col = lax.broadcasted_iota(jnp.int32, work_ref.shape, 1)
    inverse = jnp.where(row >= col, work_ref[...], 0.0)
    left_ref[...] = exact(mid, inverse, NT) * scale
    project_ref[...] = exact(inverse, cross, NT)


def factored(mid_sum, gram_left, scale, rank_width):
    sketch_width = mid_sum.size // rank_width
    return pl.pallas_call(
        functools.partial(factor_kernel, scale),
        out_shape=(
            jax.ShapeDtypeStruct((rank_width, sketch_width), F32),
            jax.ShapeDtypeStruct((sketch_width, rank_width), F32),
        ),
        scratch_shapes=[pltpu.VMEM((sketch_width, sketch_width), F32)],
        name="factor",
    )(mid_sum, gram_left)


def gram_kernel(rows_hbm, out_ref, rows_ref, sum_ref, sems):
    count, depth = rows_ref.shape
    half = depth // 2
    part = count // STEPS

    def copy_of(k):
        lines = pl.ds(pl.multiple_of(k * part, part), part)
        return lines, pltpu.make_async_copy(rows_hbm.at[lines], rows_ref.at[lines], sems.at[k])

    for k in range(STEPS):
        copy_of(k)[1].start()
    sum_ref[...] = jnp.zeros_like(sum_ref)

    def run(k, carry):
        lines, copy = copy_of(k)
        copy.wait()
        high, low = halves(rows_ref[lines, :])
        first = (high[:, :half], low[:, :half])
        second = (high[:, half:], low[:, half:])
        sum_ref[:half, :] += dot3(first, (high, low), TN)
        corner = dot3(second, second, TN)
        sum_ref[half:, :half] += corner[: half // 2]
        sum_ref[half:, half:] += corner[half // 2 :]
        return carry

    lax.fori_loop(0, STEPS, run, 0)
    spread(out_ref, sum_ref[...])


def packed_gram(rows):
    depth = rows.shape[1]
    sums = (depth // 2 + depth // 4, depth)
    peers = lax.axis_size(CUTS)
    shape = (peers, sums[0] * sums[1] // LANES // peers, LANES)
    return pl.pallas_call(
        gram_kernel,
        in_specs=[IN_HBM],
        out_specs=IN_VMEM,
        out_shape=jax.ShapeDtypeStruct(shape, F32),
        scratch_shapes=[pltpu.VMEM(rows.shape, F32), pltpu.VMEM(sums, F32), pltpu.SemaphoreType.DMA((STEPS,))],
        name="gram",
    )(rows)


def apply_kernel(rows_ref, right_ref, out_ref):
    out_ref[...] = dot3(halves(rows_ref[...]), halves(right_ref[...]), NN)


def apply_right(rows, right):
    count, depth = rows.shape
    width = right.shape[1]
    group = 512
    return pl.pallas_call(
        apply_kernel,
        grid=(count // group,),
        in_specs=[pl.BlockSpec((group, depth), lambda g: (g, 0)), whole_block(right.shape)],
        out_specs=pl.BlockSpec((group, width), lambda g: (g, 0)),
        out_shape=jax.ShapeDtypeStruct((count, width), F32),
        name="ortho",
    )(rows, right)


def project_kernel(pieces, rank_ref, project_ref, *refs):
    count = sum(pieces)
    blocks_hbm, out_hbm, block_refs, (out_ref, in_sems, out_sems) = refs[:count], refs[count], refs[count + 1 : -3], refs[-3:]
    slices = blocks_hbm[0].shape[0]
    rows = project_ref.shape[0]
    ranks = len(pieces)
    groups = slices // TILE
    slabs = [pl.ds(g * TILE, TILE) for g in range(groups)]
    arriving = [
        [
            started(hbm.at[slabs[g]], ref.at[slabs[g]], in_sems.at[g * count + n])
            for n, (hbm, ref) in enumerate(zip(blocks_hbm, block_refs))
        ]
        for g in range(groups)
    ]
    project = halves(
        jnp.concatenate(
            [project_ref[:, pl.ds(own_block(rank_ref, ranks - distance, ranks), LANES)] for distance in range(ranks)],
            axis=1,
        )
    )
    leaving = []
    for g in range(groups):
        for copy in arriving[g]:
            copy.wait()
        out = out_ref.at[g].reshape(rows * TILE, LANES)
        for i in range(0, TILE, 2):
            pair = [jnp.concatenate([ref[g * TILE + i + d] for ref in block_refs], axis=0) for d in range(2)]
            product = dot3(project, halves(jnp.concatenate(pair, axis=1)), NN)
            for d in range(2):
                out[pl.ds(i + d, rows, stride=TILE), :] = product[:, d * LANES : (d + 1) * LANES]
        leaving.append(started(out_ref.at[g], out_hbm.at[:, slabs[g]], out_sems.at[g]))
    for copy in leaving:
        copy.wait()


def projected(rank, project, stepped, pieces):
    slices = stepped[0].shape[0]
    rows = project.shape[0]
    groups = slices // TILE
    return pl.pallas_call(
        functools.partial(project_kernel, pieces),
        in_specs=[SCALAR, IN_VMEM, *[IN_HBM] * len(stepped)],
        out_specs=IN_HBM,
        out_shape=jax.ShapeDtypeStruct((rows, slices, LANES), F32),
        scratch_shapes=[
            *[pltpu.VMEM(block.shape, F32) for block in stepped],
            pltpu.VMEM((groups, rows, TILE, LANES), F32),
            pltpu.SemaphoreType.DMA((groups * len(stepped),)),
            pltpu.SemaphoreType.DMA((groups,)),
        ],
        name="project",
    )(rank, project, *stepped)


def summed(pieces, axes):
    return jnp.sum(lax.all_to_all(pieces, axes, 0, 0, tiled=True), axis=0)


def copies_of(piece, axes):
    copies = jnp.broadcast_to(piece, (lax.axis_size(axes), *piece.shape))
    return lax.all_to_all(copies, axes, 0, 0, tiled=True)


def shifted(array, distance):
    count = lax.axis_size("rank")
    return lax.ppermute(array, "rank", [(i, (i + distance) % count) for i in range(count)])


def neighbours(core):
    count = lax.axis_size(CUTS)
    head, tail = core[:, 0, :], core[:, -1, :]
    below = lax.ppermute(tail, CUTS, [(i, i + 1) for i in range(count - 1)])
    above = lax.ppermute(head, CUTS, [(i + 1, i) for i in range(count - 1)])
    return below, above


def step(core_left, core_mid, core_right, sketch_mid, sketch_right, tail_sketch, stencil):
    row_count, slices, rank_width = core_left.shape
    sketch_width = tail_sketch.shape[1]
    quarters = rank_width // LANES
    ranks = lax.axis_size("rank")
    flat_left = core_left.reshape(row_count * slices, rank_width)

    rank = lax.axis_index("rank").astype(jnp.int32).reshape(1)

    below, above = neighbours(core_mid)
    stepped = step_core(rank, core_mid, below, above, stencil, PIECES)
    own, up, far_up, far_down, down = stepped
    up = shifted(up, 1)
    down = shifted(down, -1)
    far_up = shifted(far_up, 1)
    far_down = shifted(far_down, -1)
    far_up = shifted(far_up, 1)
    far_down = shifted(far_down, -1)

    gram_left = packed_gram(flat_left)
    gram_left = summed(gram_left, CUTS)
    gram_left = sum([shifted(gram_left, d) for d in range(1, ranks)], gram_left)
    gram_left = copies_of(gram_left, CUTS)

    right_part = contract_back(rank, [core_right], (), tail_sketch, sketch_right)
    right_sum = summed(right_part, CUTS)
    right_sum = copies_of(right_sum, EVERY)

    mid_part = contract_back(rank, stepped, PIECES, right_sum, sketch_mid)
    mid_sum = summed(mid_part, CUTS)
    mid_sum = copies_of(mid_sum, EVERY)

    scale = math.sqrt(rank_width * slices * lax.axis_size(CUTS))
    left, project = factored(mid_sum, gram_left, scale, rank_width)
    product = projected(rank, project, [own, up, far_up, far_down, down], PIECES)
    blocks = product.reshape(ranks, sketch_width // ranks, slices, LANES)
    arrived = lax.all_to_all(blocks, "rank", 0, 0, tiled=True)
    next_core = jnp.moveaxis(arrived, 0, 2).reshape(sketch_width // ranks, slices, quarters * LANES)
    ortho_core = apply_right(flat_left, left).reshape(row_count, slices, sketch_width)
    return ortho_core, next_core


def solution(mesh):
    split = Mesh(
        mesh.devices.reshape(4, 4, 2, mesh.shape["rank"]), ("cuts_0", "cuts_1", "cuts_2", "rank")
    )
    in_specs = (
        P("rank", CUTS, None),
        P("rank", CUTS, None),
        P("rank", CUTS, None),
        P(None, CUTS, None),
        P(None, CUTS, None),
        P(),
        P(None, CUTS),
    )
    out_specs = (P("rank", CUTS, None), P("rank", CUTS, None))
    return jax.shard_map(step, mesh=split, in_specs=in_specs, out_specs=out_specs, check_vma=False)
```

```python
import functools
import math

import jax
import jax.numpy as jnp
from jax import lax
from jax.experimental import pallas as pl
from jax.experimental.pallas import tpu as pltpu
from jax.sharding import Mesh
from jax.sharding import PartitionSpec as P

CUTS = ("cuts_0", "cuts_1", "cuts_2")
EVERY = ("rank", "cuts_0", "cuts_1", "cuts_2")
HIGHEST = lax.Precision.HIGHEST
F32 = jnp.float32
BF16 = jnp.bfloat16
LANES = 128
TILE = 8
BLOCK = 64
PIECES = (1, 1, 2, 1)
STEPS = 4

NN = (((1,), (0,)), ((), ()))
NT = (((1,), (1,)), ((), ()))
TN = (((0,), (0,)), ((), ()))


def halves(x):
    high = x.astype(BF16)
    return high, (x - high.astype(F32)).astype(BF16)


def dot3(a, b, dims):
    (ah, al), (bh, bl) = a, b
    dot = functools.partial(lax.dot_general, dimension_numbers=dims, preferred_element_type=F32)
    return dot(ah, bh) + (dot(ah, bl) + dot(al, bh))


def exact(a, b, dims):
    return lax.dot_general(a, b, dims, precision=HIGHEST, preferred_element_type=F32)


def whole_block(shape):
    return pl.BlockSpec(shape, lambda *_: (0,) * len(shape))


def own_block(rank_ref, distance, ranks):
    return pl.multiple_of(lax.rem(rank_ref[0] + distance, ranks) * LANES, LANES)


def spread(out_ref, total):
    peers, height, _ = out_ref.shape
    out = out_ref.reshape(peers * height, LANES)
    lines = total.shape[0] // peers
    for h in range(total.shape[1] // LANES):
        for j in range(lines):
            block = total[j * peers : (j + 1) * peers, h * LANES : (h + 1) * LANES]
            out[pl.ds(h * lines + j, peers, stride=height), :] = block


def gathered(ref, peers, lines, first=0):
    count, height, _ = ref.shape
    flat = ref.reshape(count * height, LANES)
    return jnp.concatenate(
        [
            jnp.concatenate(
                [flat[pl.ds(first * height + h * lines + j, peers, stride=height), :] for h in range(height // lines)],
                axis=1,
            )
            for j in range(lines)
        ],
        axis=0,
    )


def started(source, target, sem):
    copy = pltpu.make_async_copy(source, target, sem)
    copy.start()
    return copy


def contract_kernel(core_parts, rank_ref, part_ref, *refs):
    count = sum(core_parts) if core_parts else 1
    core_hbm, sketch_hbm, out_ref, *refs = refs[:count], refs[count], refs[count + 1], *refs[count + 2 :]
    core_refs, (sketch_ref, applied_ref, core_sems, sketch_sems) = refs[:count], refs[count:]
    peers = out_ref.shape[0]
    pieces, groups, sketch_rows = sketch_ref.shape[:3]
    slices = groups * TILE
    rows = applied_ref.shape[1] // slices
    step = core_refs[0].shape[0] // STEPS

    arriving = []
    for k in range(STEPS):
        lines = pl.ds(k * step, step)
        for n, (hbm, ref) in enumerate(zip(core_hbm, core_refs)):
            arriving.append((k, started(hbm.at[lines], ref.at[lines], core_sems.at[k * count + n])))
    sketches_arriving = [
        started(
            sketch_hbm.at[:, pl.ds(g * TILE, TILE), pl.ds(h * LANES, LANES)],
            sketch_ref.at[h, g],
            sketch_sems.at[g * pieces + h],
        )
        for g in range(groups)
        for h in range(pieces)
    ]

    if core_parts:
        blocks = [lax.rem(rank_ref[0] + distance, len(core_parts)) for distance in range(len(core_parts))]
        part = jnp.concatenate([gathered(part_ref, peers, LANES // peers, block * peers) for block in blocks], axis=0)
    else:
        part = part_ref[...]
    part = halves(part)
    for k in range(STEPS):
        for chunk, copy in arriving:
            if chunk == k:
                copy.wait()
        if core_parts:
            slabs = []
            for i in range(k * step, (k + 1) * step):
                taken, blocks = list(core_refs), []
                for split in core_parts:
                    block = [taken.pop(0)[i] for _ in range(split)]
                    blocks.append(block[0] if split == 1 else jnp.concatenate(block, axis=0))
                slabs.append(jnp.concatenate(blocks, axis=1))
            core = jnp.concatenate(slabs, axis=0)
        else:
            core = core_refs[0][pl.ds(k * step, step)].reshape(step * slices, -1)
        applied = dot3(halves(core), part, NN)
        for h in range(pieces):
            own = applied[:, h * LANES : (h + 1) * LANES]
            if core_parts:
                applied_ref[h, pl.ds(k * step * rows, step * rows), :] = own
                continue
            own = own.reshape(step, groups, TILE, LANES)
            for g in range(groups):
                begin = (g * rows + k * step) * TILE
                applied_ref[h, pl.ds(begin, step * TILE), :] = own[:, g].reshape(step * TILE, LANES)
    for copy in sketches_arriving:
        copy.wait()

    def run(g, total):
        for i in range(TILE):
            if core_parts:
                lines = pl.ds(pl.multiple_of((g * TILE + i) * rows, rows), rows)
            else:
                lines = pl.ds(g * rows * TILE + i, rows, stride=TILE)
            left = [applied_ref.at[h][lines, :] for h in range(pieces)]
            right = [
                sketch_ref.at[h, g].reshape(sketch_rows * TILE, LANES)[pl.ds(i, sketch_rows, stride=TILE), :]
                for h in range(pieces)
            ]
            total += dot3(halves(jnp.concatenate(left, axis=1)), halves(jnp.concatenate(right, axis=1)), NT)
        return total

    spread(out_ref, lax.fori_loop(0, groups, run, jnp.zeros((rows, sketch_rows), F32)))


SCALAR = pl.BlockSpec(memory_space=pltpu.SMEM)
IN_VMEM = pl.BlockSpec(memory_space=pltpu.VMEM)
IN_HBM = pl.BlockSpec(memory_space=pltpu.HBM)


def contract_back(rank, cores, core_parts, part, sketch):
    sketch_rows, slices, sketch_cols = sketch.shape
    rows = cores[0].shape[1 if core_parts else 0]
    pieces = sketch_cols // LANES
    peers = lax.axis_size(CUTS)
    shape = (peers, rows * sketch_rows // LANES // peers, LANES)
    return pl.pallas_call(
        functools.partial(contract_kernel, core_parts),
        in_specs=[SCALAR, IN_VMEM, *[IN_HBM] * (len(cores) + 1)],
        out_specs=IN_VMEM,
        out_shape=jax.ShapeDtypeStruct(shape, F32),
        scratch_shapes=[
            *[pltpu.VMEM(core.shape, F32) for core in cores],
            pltpu.VMEM((pieces, slices // TILE, sketch_rows, TILE, LANES), F32),
            pltpu.VMEM((pieces, rows * slices, LANES), F32),
            pltpu.SemaphoreType.DMA((STEPS * len(cores),)),
            pltpu.SemaphoreType.DMA((pieces * slices // TILE,)),
        ],
        name="contract",
    )(rank, part, *cores, sketch)


def stencil_kernel(pieces, rank_ref, coef_ref, core_hbm, below_ref, above_ref, *refs):
    count = sum(pieces)
    outs_hbm, core_ref, step_refs, (in_sems, out_sems) = refs[:count], refs[count], refs[count + 1 : -2], refs[-2:]
    groups, blocks, rows, _, _ = core_ref.shape
    slices = groups * TILE
    arriving = [
        [
            started(
                core_hbm.at[:, pl.ds(g * TILE, TILE), pl.ds(own_block(rank_ref, distance, blocks), LANES)],
                core_ref.at[g, distance],
                in_sems.at[g * blocks + distance],
            )
            for g in range(groups)
        ]
        for distance in range(blocks)
    ]
    leaving, at = [], 0
    for distance, split in enumerate(pieces):
        for copy in arriving[distance]:
            copy.wait()
        cols = pl.ds(own_block(rank_ref, distance, blocks), LANES)

        def slab(i, distance=distance, cols=cols):
            if i < 0:
                return below_ref[:, cols]
            if i == slices:
                return above_ref[:, cols]
            flat = core_ref.at[i // TILE, distance].reshape(rows * TILE, LANES)
            return flat[pl.ds(i % TILE, rows, stride=TILE), :]

        below, core = slab(-1), slab(0)
        part = rows // split
        for i in range(slices):
            above = slab(i + 1)
            stepped = coef_ref[0, i] * below + coef_ref[1, i] * core + coef_ref[2, i] * above
            for n in range(split):
                step_refs[at + n][i] = stepped[n * part : (n + 1) * part]
            below, core = core, above
        for n in range(split):
            leaving.append(started(step_refs[at + n], outs_hbm[at + n], out_sems.at[at + n]))
        at += split
    for copy in leaving:
        copy.wait()


def step_core(rank, core, below, above, stencil, pieces):
    rows, slices, _ = core.shape
    groups, blocks = slices // TILE, len(pieces)
    shapes = [(slices, rows // split, LANES) for split in pieces for _ in range(split)]
    return pl.pallas_call(
        functools.partial(stencil_kernel, pieces),
        in_specs=[SCALAR, SCALAR, IN_HBM, IN_VMEM, IN_VMEM],
        out_specs=[IN_HBM] * len(shapes),
        out_shape=[jax.ShapeDtypeStruct(shape, F32) for shape in shapes],
        scratch_shapes=[
            pltpu.VMEM((groups, blocks, rows, TILE, LANES), F32),
            *[pltpu.VMEM(shape, F32) for shape in shapes],
            pltpu.SemaphoreType.DMA((groups * blocks,)),
            pltpu.SemaphoreType.DMA((len(shapes),)),
        ],
        name="stencil",
    )(rank, stencil, core, below, above)


def invert_factor(work_ref):
    size = work_ref.shape[0]
    lane_tiles = size // LANES
    sub = lax.broadcasted_iota(jnp.int32, (TILE, LANES), 0)
    lane = lax.broadcasted_iota(jnp.int32, (TILE, LANES), 1)
    for block in range(0, size, BLOCK):
        count = BLOCK // TILE
        tiles = [
            [work_ref[pl.ds(block + t * TILE, TILE), pl.ds(h * LANES, LANES)] for h in range(lane_tiles)]
            for t in range(count)
        ]
        for p in range(count):
            k = block + p * TILE
            home, at = divmod(k, LANES)
            cols = {
                (t, j): jnp.broadcast_to(tiles[t][home][:, at + j : at + j + 1], (TILE, LANES))
                for t in range(p, count)
                for j in range(TILE)
            }
            inside = (lane >= at) & (lane < at + TILE)
            for t in range(p, count):
                fresh = jnp.where(lane - at == sub, 1.0, 0.0) if t == p else jnp.zeros((TILE, LANES), F32)
                tiles[t][home] = jnp.where(inside, fresh, tiles[t][home])
            for j in range(TILE):

                def row(x, j=j):
                    return jnp.broadcast_to(x[j : j + 1, :], (TILE, LANES))

                scale = lax.rsqrt(row(cols[p, j]))
                pivots = {jj: row(cols[p, jj]) * scale for jj in range(j + 1, TILE)}
                lines = [row(tiles[p][h]) * scale for h in range(lane_tiles)]
                for t in range(p, count):
                    m = cols[t, j] * scale
                    if t == p:
                        m = jnp.where(sub > j, m, 0.0)
                    for jj in range(j + 1, TILE):
                        cols[t, jj] = cols[t, jj] - m * pivots[jj]
                    for h in range(lane_tiles):
                        new = tiles[t][h] - m * lines[h]
                        tiles[t][h] = jnp.where(sub == j, lines[h], new) if t == p else new
        for t in range(count):
            for h in range(lane_tiles):
                work_ref[pl.ds(block + t * TILE, TILE), pl.ds(h * LANES, LANES)] = tiles[t][h]
        end = block + BLOCK
        if end < size:
            done = work_ref[pl.ds(block, BLOCK), :]
            col = lax.broadcasted_iota(jnp.int32, (size, size), 1)
            own_row = lax.broadcasted_iota(jnp.int32, (BLOCK, size), 0) + block
            own_col = lax.broadcasted_iota(jnp.int32, (BLOCK, size), 1)
            change = exact(done, jnp.where((own_col > own_row) & (own_col < end), 0.0, done), TN)
            rest = jnp.where((col >= block) & (col < end), 0.0, work_ref[...])
            rest = rest - change
            work_ref[pl.ds(end, size - end), :] = rest[end:, :]


def factor_kernel(scale, mid_ref, gram_ref, left_ref, project_ref, work_ref):
    peers, height, _ = gram_ref.shape
    rank_width = left_ref.shape[0]
    ranks = mid_ref.shape[0] // peers
    lines = rank_width // ranks // peers
    mid = jnp.concatenate([gathered(mid_ref, peers, lines, r * peers) for r in range(ranks)], axis=0)
    gram_ref = gathered(gram_ref, peers, height * LANES // rank_width)
    half = mid.shape[0] // 2
    upper, lower = mid[:half], mid[half:]
    side = gram_ref[:half, half:]
    corner = jnp.concatenate([gram_ref[half:, :half], gram_ref[half:, half:]], axis=0)
    cross = jnp.concatenate(
        [
            exact(gram_ref[:half, :half], upper, NN) + exact(side, lower, NN),
            exact(side, upper, TN) + exact(corner, lower, NN),
        ],
        axis=0,
    )
    work_ref[...] = exact(mid, cross, TN)
    invert_factor(work_ref)
    row = lax.broadcasted_iota(jnp.int32, work_ref.shape, 0)
    col = lax.broadcasted_iota(jnp.int32, work_ref.shape, 1)
    inverse = jnp.where(row >= col, work_ref[...], 0.0)
    inverse = halves(inverse)
    left_ref[...] = dot3(halves(mid), inverse, NT) * scale
    project_ref[...] = dot3(inverse, halves(cross), NT)


def factored(mid_sum, gram_left, scale, rank_width):
    sketch_width = mid_sum.size // rank_width
    return pl.pallas_call(
        functools.partial(factor_kernel, scale),
        out_shape=(
            jax.ShapeDtypeStruct((rank_width, sketch_width), F32),
            jax.ShapeDtypeStruct((sketch_width, rank_width), F32),
        ),
        scratch_shapes=[pltpu.VMEM((sketch_width, sketch_width), F32)],
        name="factor",
    )(mid_sum, gram_left)


def gram_kernel(rows_hbm, out_ref, rows_ref, sum_ref, sems):
    count, depth = rows_ref.shape
    half = depth // 2
    part = count // STEPS

    def copy_of(k):
        lines = pl.ds(pl.multiple_of(k * part, part), part)
        return lines, pltpu.make_async_copy(rows_hbm.at[lines], rows_ref.at[lines], sems.at[k])

    for k in range(STEPS):
        copy_of(k)[1].start()
    sum_ref[...] = jnp.zeros_like(sum_ref)

    def run(k, carry):
        lines, copy = copy_of(k)
        copy.wait()
        high, low = halves(rows_ref[lines, :])
        first = (high[:, :half], low[:, :half])
        second = (high[:, half:], low[:, half:])
        sum_ref[:half, :] += dot3(first, (high, low), TN)
        corner = dot3(second, second, TN)
        sum_ref[half:, :half] += corner[: half // 2]
        sum_ref[half:, half:] += corner[half // 2 :]
        return carry

    lax.fori_loop(0, STEPS, run, 0)
    spread(out_ref, sum_ref[...])


def packed_gram(rows):
    depth = rows.shape[1]
    sums = (depth // 2 + depth // 4, depth)
    peers = lax.axis_size(CUTS)
    shape = (peers, sums[0] * sums[1] // LANES // peers, LANES)
    return pl.pallas_call(
        gram_kernel,
        in_specs=[IN_HBM],
        out_specs=IN_VMEM,
        out_shape=jax.ShapeDtypeStruct(shape, F32),
        scratch_shapes=[pltpu.VMEM(rows.shape, F32), pltpu.VMEM(sums, F32), pltpu.SemaphoreType.DMA((STEPS,))],
        name="gram",
    )(rows)


def apply_kernel(rows_ref, right_ref, out_ref):
    out_ref[...] = dot3(halves(rows_ref[...]), halves(right_ref[...]), NN)


def apply_right(rows, right):
    count, depth = rows.shape
    width = right.shape[1]
    group = 512
    return pl.pallas_call(
        apply_kernel,
        grid=(count // group,),
        in_specs=[pl.BlockSpec((group, depth), lambda g: (g, 0)), whole_block(right.shape)],
        out_specs=pl.BlockSpec((group, width), lambda g: (g, 0)),
        out_shape=jax.ShapeDtypeStruct((count, width), F32),
        name="ortho",
    )(rows, right)


def project_kernel(pieces, rank_ref, project_ref, *refs):
    count = sum(pieces)
    blocks_hbm, out_hbm, block_refs, (out_ref, in_sems, out_sems) = refs[:count], refs[count], refs[count + 1 : -3], refs[-3:]
    slices = blocks_hbm[0].shape[0]
    rows = project_ref.shape[0]
    ranks = len(pieces)
    groups = slices // TILE
    slabs = [pl.ds(g * TILE, TILE) for g in range(groups)]
    arriving = [
        [
            started(hbm.at[slabs[g]], ref.at[slabs[g]], in_sems.at[g * count + n])
            for n, (hbm, ref) in enumerate(zip(blocks_hbm, block_refs))
        ]
        for g in range(groups)
    ]
    project = halves(
        jnp.concatenate(
            [project_ref[:, pl.ds(own_block(rank_ref, ranks - distance, ranks), LANES)] for distance in range(ranks)],
            axis=1,
        )
    )
    leaving = []
    for g in range(groups):
        for copy in arriving[g]:
            copy.wait()
        out = out_ref.at[g].reshape(rows * TILE, LANES)
        for i in range(0, TILE, 2):
            pair = [jnp.concatenate([ref[g * TILE + i + d] for ref in block_refs], axis=0) for d in range(2)]
            product = dot3(project, halves(jnp.concatenate(pair, axis=1)), NN)
            for d in range(2):
                out[pl.ds(i + d, rows, stride=TILE), :] = product[:, d * LANES : (d + 1) * LANES]
        leaving.append(started(out_ref.at[g], out_hbm.at[:, slabs[g]], out_sems.at[g]))
    for copy in leaving:
        copy.wait()


def projected(rank, project, stepped, pieces):
    slices = stepped[0].shape[0]
    rows = project.shape[0]
    groups = slices // TILE
    return pl.pallas_call(
        functools.partial(project_kernel, pieces),
        in_specs=[SCALAR, IN_VMEM, *[IN_HBM] * len(stepped)],
        out_specs=IN_HBM,
        out_shape=jax.ShapeDtypeStruct((rows, slices, LANES), F32),
        scratch_shapes=[
            *[pltpu.VMEM(block.shape, F32) for block in stepped],
            pltpu.VMEM((groups, rows, TILE, LANES), F32),
            pltpu.SemaphoreType.DMA((groups * len(stepped),)),
            pltpu.SemaphoreType.DMA((groups,)),
        ],
        name="project",
    )(rank, project, *stepped)


def summed(pieces, axes):
    return jnp.sum(lax.all_to_all(pieces, axes, 0, 0, tiled=True), axis=0)


def copies_of(piece, axes):
    copies = jnp.broadcast_to(piece, (lax.axis_size(axes), *piece.shape))
    return lax.all_to_all(copies, axes, 0, 0, tiled=True)


def shifted(array, distance):
    count = lax.axis_size("rank")
    return lax.ppermute(array, "rank", [(i, (i + distance) % count) for i in range(count)])


def neighbours(core):
    count = lax.axis_size(CUTS)
    head, tail = core[:, 0, :], core[:, -1, :]
    below = lax.ppermute(tail, CUTS, [(i, i + 1) for i in range(count - 1)])
    above = lax.ppermute(head, CUTS, [(i + 1, i) for i in range(count - 1)])
    return below, above


def step(core_left, core_mid, core_right, sketch_mid, sketch_right, tail_sketch, stencil):
    row_count, slices, rank_width = core_left.shape
    sketch_width = tail_sketch.shape[1]
    quarters = rank_width // LANES
    ranks = lax.axis_size("rank")
    flat_left = core_left.reshape(row_count * slices, rank_width)

    rank = lax.axis_index("rank").astype(jnp.int32).reshape(1)

    below, above = neighbours(core_mid)
    stepped = step_core(rank, core_mid, below, above, stencil, PIECES)
    own, up, far_up, far_down, down = stepped
    up = shifted(up, 1)
    down = shifted(down, -1)
    far_up = shifted(far_up, 1)
    far_down = shifted(far_down, -1)
    far_up = shifted(far_up, 1)
    far_down = shifted(far_down, -1)

    gram_left = packed_gram(flat_left)
    right_part = contract_back(rank, [core_right], (), tail_sketch, sketch_right)
    height = right_part.shape[1]
    sums = summed(jnp.concatenate([right_part, gram_left], axis=1), CUTS)
    right_sum, gram_left = sums[:height], sums[height:]
    gram_left = sum([shifted(gram_left, d) for d in range(1, ranks)], gram_left)
    gram_left = copies_of(gram_left, CUTS)
    right_sum = copies_of(right_sum, EVERY)

    mid_part = contract_back(rank, stepped, PIECES, right_sum, sketch_mid)
    mid_sum = summed(mid_part, CUTS)
    mid_sum = copies_of(mid_sum, EVERY)

    scale = math.sqrt(rank_width * slices * lax.axis_size(CUTS))
    left, project = factored(mid_sum, gram_left, scale, rank_width)
    product = projected(rank, project, [own, up, far_up, far_down, down], PIECES)
    blocks = product.reshape(ranks, sketch_width // ranks, slices, LANES)
    arrived = lax.all_to_all(blocks, "rank", 0, 0, tiled=True)
    next_core = jnp.moveaxis(arrived, 0, 2).reshape(sketch_width // ranks, slices, quarters * LANES)
    ortho_core = apply_right(flat_left, left).reshape(row_count, slices, sketch_width)
    return ortho_core, next_core


def solution(mesh):
    split = Mesh(
        mesh.devices.reshape(4, 4, 2, mesh.shape["rank"]), ("cuts_0", "cuts_1", "cuts_2", "rank")
    )
    in_specs = (
        P("rank", CUTS, None),
        P("rank", CUTS, None),
        P("rank", CUTS, None),
        P(None, CUTS, None),
        P(None, CUTS, None),
        P(),
        P(None, CUTS),
    )
    out_specs = (P("rank", CUTS, None), P("rank", CUTS, None))
    return jax.shard_map(step, mesh=split, in_specs=in_specs, out_specs=out_specs, check_vma=False)
```
